128 devices in a mesh: dp: 32 (over x, z, core), tensor: 4 (over y).
Axes of the slice: x: 4, y: 4, z: 4, core: 2. Of those that a mesh axis runs over, the one named last changes fastest.
Arguments:
- tokens: bfloat16 [16384, 4096], P(('dp', 'tensor')), may hold values from -6 to 6
- norm_gain: float32 [4096], replicated, may hold values from 0.1 to 1.9
- w_query: bfloat16 [4096, 2048], P(None, 'tensor'), may hold values from -2 to 2
- key_weight: bfloat16 [4096, 512], P(None, 'tensor'), may hold values from -0.09375 to 0.09375
- value_weight: bfloat16 [4096, 512], P(None, 'tensor'), may hold values from -0.09375 to 0.09375
- w_out: bfloat16 [2048, 4096], P('tensor'), may hold values from -0.125 to 0.125
- lengths: int32 [16], replicated, may hold values from 1 to 8704, 16384 in all
Outputs:
- layer_out: bfloat16 [16384, 4096], P(('dp', 'tensor'))
The draws below stay inside these ranges and needn't reach their ends.
Inputs may be any that keep to these rules, and one draw needn't show every extreme that they name: The lengths sum to 16384, and some document has exactly 8704 tokens.
All inputs are finite; a program needn't handle non-finite values.
Results may differ from the reference program's by a relative error of at most 0.0095.
The reference program's roundings to bfloat16 on the way count: a program that leaves them out, or rounds other values in their place, can miss the bound.
Values may be sent and summed in bfloat16 or wider, within the bound.
No kernel may reach another device: no remote copies, remote signals or barrier semaphores. Data moves between devices by JAX's collectives and lax.ppermute only.
A program may use at most 128 MiB of HBM per device.

```python
import math
import jax
import jax.numpy as jnp
import numpy as np
from jax import lax

MODEL_WIDTH = 4096
QUERY_HEADS = 16
KEY_VALUE_HEADS = 4
HEAD_SIZE = 128
DOC_MAX = 8704
TOKENS = 16384
NDOC = 16


def draw_w_query(key, part):
    folded = jax.random.fold_in(key, 7331)
    base_key, selection_key, magnitude_key = jax.random.split(folded, 3)
    width = QUERY_HEADS * HEAD_SIZE
    base = jax.random.normal(base_key, (MODEL_WIDTH, width), jnp.float32)
    group_count = QUERY_HEADS // KEY_VALUE_HEADS
    selected = jax.random.randint(selection_key, (KEY_VALUE_HEADS,), 0, group_count)
    magnitude = jnp.exp(jax.random.uniform(magnitude_key, (KEY_VALUE_HEADS,), jnp.float32, math.log(30.0), math.log(60.0)))
    head_index = jnp.arange(QUERY_HEADS, dtype=jnp.int32)
    owner = head_index // group_count
    strong = head_index % group_count == selected[owner]
    factor = jnp.where(strong, magnitude[owner], 1.0)
    columns = jnp.repeat(factor, HEAD_SIZE)
    scaled = base * MODEL_WIDTH ** (-0.5) * columns[None, :]
    return jnp.clip(scaled, -2.0, 2.0).astype(jnp.bfloat16)


def block_scale(own_key, shape, cuts, least, largest):
    factor_of, own = 1.0, jax.random.fold_in(own_key, 6)
    for position, shards_of in cuts:
        steps = jnp.exp(jax.random.uniform(jax.random.fold_in(own, position), (shards_of,), jnp.float32, least / len(cuts), largest / len(cuts)))
        factor_of = factor_of * jnp.repeat(steps, shape[position] // shards_of).reshape([-1 if axis == position else 1 for axis in range(len(shape))])
    return factor_of


def profile(number_of, total, limit, lean):
    weights = [(1 << 20) // math.isqrt(rank ** lean) + 1 for rank in range(2, number_of + 1)]
    surplus, counts = total - limit - (number_of - 1), [1] * (number_of - 1)
    while surplus > 0:
        free = [i for i in range(number_of - 1) if counts[i] < limit]
        whole, remaining = sum([weights[i] for i in free]), surplus
        for i in free:
            extra = min(limit - counts[i], max(1, remaining * weights[i] // whole), surplus)
            counts[i] = counts[i] + extra
            surplus = surplus - extra
    return np.array([limit] + counts)


def uneven_parts(key, count, total, reach, skew):
    if count == 2:
        one = jax.random.randint(key, (), max(1, total - reach), min(reach, total - 1) + 1)
        return jnp.stack([one, total - one])
    sizes = jnp.asarray(profile(count, total, reach, skew), jnp.int32)
    pairs = (count - 1) // 2
    giver, receiver = sizes[1:1 + 2 * pairs:2], sizes[2:2 + 2 * pairs:2]
    slack = jnp.minimum(giver - 1, reach - receiver)
    shifted = jax.random.randint(jax.random.fold_in(key, 1), (pairs,), 0, 1 << 20) % (slack + 1)
    sizes = sizes.at[1:1 + 2 * pairs:2].set(giver - shifted).at[2:2 + 2 * pairs:2].set(receiver + shifted)
    return sizes[jax.random.permutation(jax.random.fold_in(key, 2), count)]


def centred(own_key, extent, spread, bound, cuts=(), kind=jnp.bfloat16):
    factor_of = block_scale(own_key, extent, cuts, -0.22, 0.18) if cuts else 1.0
    entries = jax.random.normal(own_key, extent, jnp.float32) * spread * factor_of
    return jnp.minimum(jnp.maximum(entries, -bound), bound).astype(kind)


def setup_inputs(seed: int = 0) -> dict:
    key_list = jax.random.split(jax.random.key(seed), 8)
    tokens = centred(key_list[0], (TOKENS, MODEL_WIDTH), 1.0, 6.0, ((0, 128),))
    norm_gain = jnp.clip(1.0 + 0.18 * jax.random.normal(key_list[1], (MODEL_WIDTH,), jnp.float32), 0.1, 1.9)
    w_query = draw_w_query(jax.random.fold_in(key_list[7], 71), 0)
    key_weight = centred(key_list[3], (MODEL_WIDTH, KEY_VALUE_HEADS * HEAD_SIZE), MODEL_WIDTH ** -0.5, 0.09375, ((1, 4),))
    value_weight = centred(key_list[4], (MODEL_WIDTH, KEY_VALUE_HEADS * HEAD_SIZE), MODEL_WIDTH ** -0.5, 0.09375, ((1, 4),))
    w_out = centred(key_list[5], (QUERY_HEADS * HEAD_SIZE, MODEL_WIDTH), (QUERY_HEADS * HEAD_SIZE) ** -0.5, 0.125, ((0, 4),))
    lengths = uneven_parts(key_list[6], NDOC, TOKENS, DOC_MAX, 2).astype(jnp.int32)
    return {"tokens": tokens, "norm_gain": norm_gain, "w_query": w_query, "key_weight": key_weight, "value_weight": value_weight, "w_out": w_out, "lengths": lengths}


epsilon = 1e-05
rope_base = 500000.0
masked = -1e+30

def doc_starts(lengths, positions):
    doc_ends = jnp.cumsum(lengths)
    closed = (doc_ends[None, :] <= positions[:, None]).astype(jnp.int32)
    return lax.optimization_barrier(jnp.sum(closed * lengths[None, :], axis=1)).astype(jnp.int32)

def rotate(vectors, offsets):
    half_width = vectors.shape[-1] // 2
    exponent = jnp.arange(half_width, dtype=jnp.float32) * (-2.0 / vectors.shape[-1])
    frequency = rope_base ** exponent
    angles = offsets.astype(jnp.float32)[:, None] * frequency[None, :]
    cos_part = jnp.cos(angles)[:, None, :]
    sin_part = jnp.sin(angles)[:, None, :]
    leading = vectors[..., :half_width]
    trailing = vectors[..., half_width:]
    return jnp.concatenate([leading * cos_part - trailing * sin_part, trailing * cos_part + leading * sin_part], axis=-1)

def project(tokens, norm_gain, w_query, key_weight, value_weight, positions, starts):
    count = tokens.shape[0]
    wide = tokens.astype(jnp.float32)
    inverse = lax.rsqrt(lax.optimization_barrier(jnp.mean(wide * wide, axis=1, keepdims=True)) + epsilon)
    normed = (wide * inverse * norm_gain[None, :]).astype(jnp.bfloat16)
    offsets = positions - starts
    query_rows = jnp.dot(normed, w_query, preferred_element_type=jnp.float32).reshape(count, -1, HEAD_SIZE)
    query_rows = rotate(query_rows, offsets).astype(jnp.bfloat16)
    key = jnp.dot(normed, key_weight, preferred_element_type=jnp.float32).reshape(count, -1, HEAD_SIZE)
    key = rotate(key, offsets).astype(jnp.bfloat16)
    value_rows = jnp.dot(normed, value_weight, preferred_element_type=jnp.float32).astype(jnp.bfloat16)
    return (query_rows, key.reshape(count, -1), value_rows)

def reference(tokens, norm_gain, w_query, key_weight, value_weight, w_out, lengths):
    total_count = tokens.shape[0]
    positions = jnp.arange(total_count, dtype=jnp.int32)
    starts = doc_starts(lengths, positions)
    query_rows, key, value_rows = project(tokens, norm_gain, w_query, key_weight, value_weight, positions, starts)
    block_index = min(512, total_count)
    window = min(DOC_MAX + block_index, total_count)
    group_count = QUERY_HEADS // KEY_VALUE_HEADS
    query_rows = query_rows.reshape(total_count // block_index, block_index, KEY_VALUE_HEADS, group_count, HEAD_SIZE)
    key = key.reshape(total_count, KEY_VALUE_HEADS, HEAD_SIZE)
    value_rows = value_rows.reshape(total_count, KEY_VALUE_HEADS, HEAD_SIZE)
    start_blocks = starts.reshape(total_count // block_index, block_index)
    scale = HEAD_SIZE ** (-0.5)

    def attend(pieces):
        index, query_block, start_block = pieces
        first = (index * block_index).astype(jnp.int32)
        key_first = jnp.clip(first + block_index - window, 0, total_count - window).astype(jnp.int32)
        key_block = lax.dynamic_slice_in_dim(key, key_first, window, 0)
        value_block = lax.dynamic_slice_in_dim(value_rows, key_first, window, 0)
        scores = jnp.einsum('qkgd,skd->qkgs', query_block.astype(jnp.float32), key_block.astype(jnp.float32)) * scale
        key_pos = key_first + jnp.arange(window, dtype=jnp.int32)
        query_pos = first + jnp.arange(block_index, dtype=jnp.int32)
        visible = (key_pos[None, :] >= start_block[:, None]) & (key_pos[None, :] <= query_pos[:, None])
        scores = jnp.where(visible[:, None, None, :], scores, masked)
        peak = lax.optimization_barrier(jnp.max(scores, axis=-1, keepdims=True))
        probs = jnp.exp(scores - peak)
        mass = lax.optimization_barrier(jnp.sum(probs, axis=-1, keepdims=True))
        weights = lax.optimization_barrier(probs.astype(jnp.bfloat16)).astype(jnp.float32)
        mixed = jnp.einsum('qkgs,skd->qkgd', weights, value_block.astype(jnp.float32)) / mass
        return mixed.reshape(block_index, QUERY_HEADS * HEAD_SIZE).astype(jnp.bfloat16)
    blocks = jnp.arange(total_count // block_index, dtype=jnp.int32)
    attended = lax.map(attend, (blocks, query_rows, start_blocks)).reshape(total_count, QUERY_HEADS * HEAD_SIZE)
    branch = jnp.dot(attended, w_out, preferred_element_type=jnp.float32)
    return (tokens.astype(jnp.float32) + branch).astype(jnp.bfloat16)
```

```python
import functools

import jax
import jax.numpy as jnp
from jax import lax
from jax.experimental import pallas as pl
from jax.experimental.pallas import tpu as pltpu
from jax.sharding import PartitionSpec as P

HEAD_SIZE = 128


epsilon = 1e-05
rope_base = 500000.0
masked = -1e30
initial_peak = -1e29
KEY_BLOCK = 1024
ROWS = 256
exp2_scale = 1.4426950408889634 * HEAD_SIZE ** (-0.5)


def doc_starts(lengths, positions):
    doc_ends = jnp.cumsum(lengths)
    closed = (doc_ends[None, :] <= positions[:, None]).astype(jnp.int32)
    return jnp.sum(closed * lengths[None, :], axis=1)


def rotate(vectors, offsets):
    half_width = vectors.shape[-1] // 2
    exponent = jnp.arange(half_width, dtype=jnp.float32) * (-2.0 / vectors.shape[-1])
    frequency = rope_base**exponent
    angles = offsets.astype(jnp.float32)[:, None] * frequency[None, :]
    cos_part = jnp.cos(angles)[:, None, :]
    sin_part = jnp.sin(angles)[:, None, :]
    leading = vectors[..., :half_width]
    trailing = vectors[..., half_width:]
    return jnp.concatenate(
        [leading * cos_part - trailing * sin_part, trailing * cos_part + leading * sin_part],
        axis=-1,
    )


def project(tokens, norm_gain, w_query, key_weight, value_weight, positions, starts):
    count = tokens.shape[0]
    wide = tokens.astype(jnp.float32)
    inverse = lax.rsqrt(jnp.mean(wide * wide, axis=1, keepdims=True) + epsilon)
    normed = (wide * inverse * norm_gain[None, :]).astype(jnp.bfloat16)
    offsets = positions - starts
    query_rows = jnp.dot(normed, w_query, preferred_element_type=jnp.float32).reshape(
        count, -1, HEAD_SIZE
    )
    query_rows = rotate(query_rows, offsets).astype(jnp.bfloat16)
    key = jnp.dot(normed, key_weight, preferred_element_type=jnp.float32).reshape(
        count, -1, HEAD_SIZE
    )
    key = rotate(key, offsets).astype(jnp.bfloat16)
    value_rows = jnp.dot(normed, value_weight, preferred_element_type=jnp.float32).astype(
        jnp.bfloat16
    )
    return (query_rows.reshape(count, -1), key.reshape(count, -1), value_rows)


def attend_kernel(bounds, query, starts, kv, out, rows, peak, summed):
    first, low, high, full_low, full_high = [bounds[i] for i in range(5)]
    count = query.shape[0]
    heads = query.shape[1] // HEAD_SIZE
    size = KEY_BLOCK
    for h in range(heads):
        rows[h * count : (h + 1) * count, :] = query[:, h * HEAD_SIZE : (h + 1) * HEAD_SIZE]
    peak[...] = jnp.full(peak.shape, initial_peak, jnp.float32)
    summed[...] = jnp.zeros(summed.shape, jnp.float32)

    def step(index, cut):
        offset = pl.multiple_of(index * size, size)
        keys = kv[pl.ds(offset, size), :HEAD_SIZE]
        values = kv[pl.ds(offset, size), HEAD_SIZE:]
        values = jnp.concatenate([values, jnp.ones((size, HEAD_SIZE), jnp.bfloat16)], axis=1)
        for r in range(heads * count // ROWS):
            at = slice(r * ROWS, (r + 1) * ROWS)
            scores = lax.dot_general(
                rows[at, :], keys, (((1,), (1,)), ((), ())), preferred_element_type=jnp.float32
            )
            if cut:
                local = (r * ROWS) % count
                here = slice(local, local + ROWS)
                key_pos = offset + lax.broadcasted_iota(jnp.int32, (ROWS, size), 1)
                query_pos = first + local + lax.broadcasted_iota(jnp.int32, (ROWS, size), 0)
                visible = (key_pos >= starts[here, :]) & (key_pos <= query_pos)
                scores = jnp.where(visible, scores, masked)
            parts = [scores[:, c : c + HEAD_SIZE] for c in range(0, size, HEAD_SIZE)]
            old = peak[at, :]
            best = functools.reduce(jnp.maximum, parts)
            fresh = jnp.maximum(old, jnp.max(best, axis=1, keepdims=True))
            peak[at, :] = fresh
            shrink = jnp.exp2((old - fresh) * exp2_scale)
            probs = [jnp.exp2((part - fresh) * exp2_scale).astype(jnp.bfloat16) for part in parts]
            update = jnp.dot(
                jnp.concatenate(probs, axis=1), values, preferred_element_type=jnp.float32
            )
            summed[at, :HEAD_SIZE] = summed[at, :HEAD_SIZE] * shrink + update[:, :HEAD_SIZE]
            summed[at, HEAD_SIZE:] = summed[at, HEAD_SIZE:] * shrink + update[:, HEAD_SIZE:]

    def one_block(index, carry):
        whole = (index >= full_low) & (index < full_high)

        @pl.when(whole)
        def _():
            step(index, False)

        @pl.when(jnp.logical_not(whole))
        def _():
            step(index, True)

        return carry

    lax.fori_loop(low, high, one_block, 0)
    for h in range(heads):
        at = slice(h * count, (h + 1) * count)
        attended = summed[at, :HEAD_SIZE] / summed[at, HEAD_SIZE:]
        out[:, h * HEAD_SIZE : (h + 1) * HEAD_SIZE] = attended.astype(jnp.bfloat16)


def attend(query, kv, starts, first):
    count, width = query.shape
    rows = count * width // HEAD_SIZE
    size = KEY_BLOCK
    bounds = jnp.stack(
        [
            first,
            starts[0] // size,
            (first + count - 1) // size + 1,
            (starts[-1] + size - 1) // size,
            (first + 1) // size,
        ]
    ).astype(jnp.int32)
    vmem = pl.BlockSpec(memory_space=pltpu.VMEM)
    return pl.pallas_call(
        attend_kernel,
        out_shape=jax.ShapeDtypeStruct((count, width), jnp.bfloat16),
        in_specs=[pl.BlockSpec(memory_space=pltpu.SMEM), vmem, vmem, vmem],
        out_specs=vmem,
        scratch_shapes=[
            pltpu.VMEM((rows, HEAD_SIZE), jnp.bfloat16),
            pltpu.VMEM((rows, HEAD_SIZE), jnp.float32),
            pltpu.VMEM((rows, 2 * HEAD_SIZE), jnp.float32),
        ],
        compiler_params=pltpu.CompilerParams(vmem_limit_bytes=56 * 2**20),
        cost_estimate=pl.CostEstimate(
            flops=rows * 8704 * 512, transcendentals=rows * 8704, bytes_accessed=8 << 20
        ),
        name="attend",
    )(bounds, query, starts[:, None], kv)


def body(tokens, norm_gain, w_query, key_weight, value_weight, w_out, lengths):
    gathered = lax.all_gather(tokens, "tensor", axis=0, tiled=True)
    count = gathered.shape[0]
    first = lax.axis_index("dp") * count
    positions = first + jnp.arange(count, dtype=jnp.int32)
    starts = doc_starts(lengths, positions)
    query_rows, key, value_rows = project(
        gathered, norm_gain, w_query, key_weight, value_weight, positions, starts
    )
    kv = lax.all_gather(jnp.concatenate([key, value_rows], axis=1), "dp", axis=0, tiled=True)
    attended = attend(query_rows, kv, starts, first)
    branch = lax.psum_scatter(
        jnp.dot(attended, w_out, preferred_element_type=jnp.float32).astype(jnp.bfloat16),
        "tensor",
        scatter_dimension=0,
        tiled=True,
    ).astype(jnp.float32)
    return (tokens.astype(jnp.float32) + branch).astype(jnp.bfloat16)


def solution(mesh):
    in_specs = (
        P(("dp", "tensor"), None),
        P(),
        P(None, "tensor"),
        P(None, "tensor"),
        P(None, "tensor"),
        P("tensor", None),
        P(),
    )
    out_specs = P(("dp", "tensor"), None)
    return jax.shard_map(body, mesh=mesh, in_specs=in_specs, out_specs=out_specs, check_vma=False)
```

```python
import functools

import jax
import jax.numpy as jnp
from jax import lax
from jax.experimental import pallas as pl
from jax.experimental.pallas import tpu as pltpu
from jax.sharding import PartitionSpec as P

HEAD_SIZE = 128

epsilon = 1e-05
rope_base = 500000.0
masked = -1e30
initial_peak = -1e29
ROWS = 256
exp2_scale = 1.4426950408889634 * HEAD_SIZE ** (-0.5)

RING = 4
RELATIVE = (0, 3, 1, 2)


def ring_shift(step):
    return [(i, (i + step) % RING) for i in range(RING)]


def plane_shift(step, first_axis):
    pairs = []
    for d in range(32):
        x, z, core = d // 8, d // 2 % 4, d % 2
        if (core == 0) == first_axis:
            z = (z + step) % 4
        else:
            x = (x + step) % 4
        pairs.append((d, x * 8 + z * 2 + core))
    return pairs


CORE_SWAP = [(d, d ^ 1) for d in range(32)]


def ring_gather(piece, axis, shift):
    half = piece.shape[0] // 2
    behind = lax.ppermute(piece, axis, shift(1))
    ahead = lax.ppermute(piece, axis, shift(-1))
    upper = lax.ppermute(behind[:half], axis, shift(1))
    lower = lax.ppermute(ahead[half:], axis, shift(-1))
    return [piece, behind, ahead, upper, lower]


def gather_plane(keys, values):
    core = lax.axis_index("dp") % 2
    other = lax.ppermute(jnp.where(core == 0, values, keys), "dp", CORE_SWAP)
    mine = jnp.where(
        core == 0,
        jnp.concatenate([keys, other], axis=0),
        jnp.concatenate([other, values], axis=0),
    )
    line = ring_gather(mine, "dp", functools.partial(plane_shift, first_axis=True))
    plane = ring_gather(
        jnp.concatenate(line, axis=0), "dp", functools.partial(plane_shift, first_axis=False)
    )
    plane = jnp.concatenate(plane, axis=0)
    swapped = lax.ppermute(plane, "dp", CORE_SWAP)
    return jnp.where(core == 0, plane, swapped), jnp.where(core == 0, swapped, plane)


def doc_starts(lengths, positions):
    doc_ends = jnp.cumsum(lengths)
    closed = (doc_ends[None, :] <= positions[:, None]).astype(jnp.int32)
    return jnp.sum(closed * lengths[None, :], axis=1)


def angles_of(offsets):
    half_width = HEAD_SIZE // 2
    exponent = jnp.arange(half_width, dtype=jnp.float32) * (-2.0 / HEAD_SIZE)
    frequency = rope_base**exponent
    angles = offsets.astype(jnp.float32)[:, None] * frequency[None, :]
    return jnp.cos(angles), jnp.sin(angles)


def rotate(vectors, cos_part, sin_part):
    count = vectors.shape[0]
    vectors = vectors.reshape(count, -1, HEAD_SIZE)
    half_width = HEAD_SIZE // 2
    cos_part, sin_part = cos_part[:, None, :], sin_part[:, None, :]
    leading = vectors[..., :half_width]
    trailing = vectors[..., half_width:]
    turned = jnp.concatenate(
        [leading * cos_part - trailing * sin_part, trailing * cos_part + leading * sin_part],
        axis=-1,
    )
    return turned.astype(jnp.bfloat16).reshape(count, -1)


def norm(tokens, norm_gain):
    wide = tokens.astype(jnp.float32)
    inverse = lax.rsqrt(jnp.mean(wide * wide, axis=1, keepdims=True) + epsilon)
    return (wide * inverse * norm_gain[None, :]).astype(jnp.bfloat16)


def wide_dot(a, b):
    return jnp.dot(a, b, preferred_element_type=jnp.float32)


def attend_kernel(
    bounds, slots, query, starts, query_at, key_at, keys, values, out, rows, peak, summed, kbuf, vbuf, sems
):
    low, high, full_low, full_high = [bounds[i] for i in range(4)]
    count = query.shape[0]
    heads = query.shape[1] // HEAD_SIZE
    size = kbuf.shape[1]

    def copies(chip):
        slot = lax.rem(chip, 2)
        k_from = pl.multiple_of(slots[0, chip] * size, size)
        v_from = pl.multiple_of(slots[1, chip] * size, size)
        return (
            pltpu.make_async_copy(keys.at[pl.ds(k_from, size)], kbuf.at[slot], sems.at[0, slot]),
            pltpu.make_async_copy(values.at[pl.ds(v_from, size)], vbuf.at[slot], sems.at[1, slot]),
        )

    for copy in copies(low):
        copy.start()
    for h in range(heads):
        rows[h * count : (h + 1) * count, :] = query[:, h * HEAD_SIZE : (h + 1) * HEAD_SIZE]
    peak[...] = jnp.full(peak.shape, initial_peak, jnp.float32)
    summed[...] = jnp.zeros(summed.shape, jnp.float32)

    def step(chip, cut):
        slot = lax.rem(chip, 2)
        block_keys = kbuf[slot]
        block_values = jnp.concatenate(
            [vbuf[slot], jnp.ones((size, HEAD_SIZE), jnp.bfloat16)], axis=1
        )
        if cut:
            where = chip * size + key_at[...]
            visible = (where >= starts[...]) & (where <= query_at[...])
            if count < ROWS:
                visible = jnp.concatenate([visible] * (ROWS // count), axis=0)
        for r in range(heads * count // ROWS):
            at = slice(r * ROWS, (r + 1) * ROWS)
            scores = lax.dot_general(
                rows[at, :], block_keys, (((1,), (1,)), ((), ())), preferred_element_type=jnp.float32
            )
            if cut:
                local = (r * ROWS) % max(count, ROWS)
                scores = jnp.where(visible[local : local + ROWS], scores, masked)
            parts = [scores[:, c : c + HEAD_SIZE] for c in range(0, size, HEAD_SIZE)]
            old = peak[at, :]
            best = functools.reduce(jnp.maximum, parts)
            fresh = jnp.maximum(old, jnp.max(best, axis=1, keepdims=True))
            peak[at, :] = fresh
            shrink = jnp.exp2((old - fresh) * exp2_scale)
            probs = [jnp.exp2((part - fresh) * exp2_scale).astype(jnp.bfloat16) for part in parts]
            update = wide_dot(jnp.concatenate(probs, axis=1), block_values)
            summed[at, :HEAD_SIZE] = summed[at, :HEAD_SIZE] * shrink + update[:, :HEAD_SIZE]
            summed[at, HEAD_SIZE:] = summed[at, HEAD_SIZE:] * shrink + update[:, HEAD_SIZE:]

    def one_block(chip, carry):
        for copy in copies(chip):
            copy.wait()

        @pl.when(chip + 1 < high)
        def _():
            for copy in copies(chip + 1):
                copy.start()

        whole = (chip >= full_low) & (chip < full_high)

        @pl.when(whole)
        def _():
            step(chip, False)

        @pl.when(jnp.logical_not(whole))
        def _():
            step(chip, True)

        return carry

    lax.fori_loop(low, high, one_block, 0)
    for h in range(heads):
        at = slice(h * count, (h + 1) * count)
        attended = summed[at, :HEAD_SIZE] / summed[at, HEAD_SIZE:]
        out[:, h * HEAD_SIZE : (h + 1) * HEAD_SIZE] = attended.astype(jnp.bfloat16)


def attend(query, starts, query_at, key_at, keys, values, slots):
    count, width = query.shape
    rows = count * width // HEAD_SIZE
    size = key_at.shape[1]
    bounds = jnp.stack(
        [
            jnp.min(starts) // size,
            jnp.max(query_at) // size + 1,
            (jnp.max(starts) + size - 1) // size,
            (jnp.min(query_at) + 1) // size,
        ]
    ).astype(jnp.int32)
    vmem = pl.BlockSpec(memory_space=pltpu.VMEM)
    smem = pl.BlockSpec(memory_space=pltpu.SMEM)
    hbm = pl.BlockSpec(memory_space=pl.ANY)
    return pl.pallas_call(
        attend_kernel,
        out_shape=jax.ShapeDtypeStruct((count, width), jnp.bfloat16),
        in_specs=[smem, smem, vmem, vmem, vmem, vmem, hbm, hbm],
        out_specs=vmem,
        scratch_shapes=[
            pltpu.VMEM((rows, HEAD_SIZE), jnp.bfloat16),
            pltpu.VMEM((rows, HEAD_SIZE), jnp.float32),
            pltpu.VMEM((rows, 2 * HEAD_SIZE), jnp.float32),
            pltpu.VMEM((2, size, HEAD_SIZE), jnp.bfloat16),
            pltpu.VMEM((2, size, HEAD_SIZE), jnp.bfloat16),
            pltpu.SemaphoreType.DMA((2, 2)),
        ],
        compiler_params=pltpu.CompilerParams(vmem_limit_bytes=40 * 2**20),
        cost_estimate=pl.CostEstimate(
            flops=rows * 4096 * 512, transcendentals=rows * 4096, bytes_accessed=4 << 20
        ),
        name="attend",
    )(bounds, slots, query, starts[:, None], query_at[:, None], key_at, keys, values)


def body(tokens, norm_gain, w_query, key_weight, value_weight, w_out, lengths):
    count = tokens.shape[0]
    dp, mine = lax.axis_index("dp"), lax.axis_index("tensor")
    own_x, own_z = dp // 8, dp // 2 % 4
    quarter = (mine + jnp.array(RELATIVE, jnp.int32)) % RING
    local = (quarter[:, None] * count + jnp.arange(count, dtype=jnp.int32)[None, :]).reshape(-1)
    positions = dp * (RING * count) + local
    starts = doc_starts(lengths, positions)
    cos_part, sin_part = angles_of(positions - starts)
    key_at = jnp.concatenate([local, local + RING * count])[None, :]
    chips = jnp.arange(16, dtype=jnp.int32)
    place = jnp.array([0, 2, 3, 1], jnp.int32)
    at_x, at_z = place[(chips // 4 - own_x) % 4], place[(chips % 4 - own_z) % 4]
    slots = jnp.stack([4 * at_x + at_z, 4 * at_z + at_x])

    own, behind, ahead, upper, lower = ring_gather(norm(tokens, norm_gain), "tensor", ring_shift)
    pieces = [own, behind, ahead, jnp.concatenate([upper, lower], axis=0)]
    query, keys, values = [], [], []
    for q, piece in enumerate(pieces):
        at = slice(q * count, (q + 1) * count)
        keys.append(rotate(wide_dot(piece, key_weight), cos_part[at], sin_part[at]))
        values.append(wide_dot(piece, value_weight).astype(jnp.bfloat16))
        query.append(rotate(wide_dot(piece, w_query), cos_part[at], sin_part[at]))
    all_keys, all_values = gather_plane(
        jnp.concatenate(keys, axis=0), jnp.concatenate(values, axis=0)
    )

    def branch(first, last, after=None):
        at = slice(first * count, last * count)
        rows = jnp.concatenate(query[first:last], axis=0)
        if after is not None:
            rows, after = lax.optimization_barrier((rows, after))
        attended = attend(
            rows, starts[at], positions[at], key_at, all_keys, all_values, slots
        )
        return wide_dot(attended, w_out), after

    half = w_out.shape[1] // 2
    far, _ = branch(3, 4)
    far = far.astype(jnp.bfloat16)
    near, far = branch(1, 3, far)
    from_behind = lax.ppermute(far[:, :half], "tensor", ring_shift(1))
    from_ahead = lax.ppermute(far[:, half:], "tensor", ring_shift(-1))
    to_behind, to_ahead = near[:count], near[count:]
    plain_up = lax.ppermute(to_ahead[:, half:].astype(jnp.bfloat16), "tensor", ring_shift(1))
    plain_down = lax.ppermute(to_behind[:, :half].astype(jnp.bfloat16), "tensor", ring_shift(-1))
    sum_up = lax.ppermute(
        (to_ahead[:, :half] + from_behind.astype(jnp.float32)).astype(jnp.bfloat16),
        "tensor",
        ring_shift(1),
    )
    sum_down = lax.ppermute(
        (to_behind[:, half:] + from_ahead.astype(jnp.float32)).astype(jnp.bfloat16),
        "tensor",
        ring_shift(-1),
    )
    here, _ = branch(0, 1, plain_up)
    wide = [a.astype(jnp.float32) for a in (sum_up, plain_down, plain_up, sum_down)]
    total = here + jnp.concatenate([wide[0] + wide[1], wide[2] + wide[3]], axis=1)
    return (tokens.astype(jnp.float32) + total).astype(jnp.bfloat16)


def solution(mesh):
    in_specs = (
        P(("dp", "tensor"), None),
        P(),
        P(None, "tensor"),
        P(None, "tensor"),
        P(None, "tensor"),
        P("tensor", None),
        P(),
    )
    out_specs = P(("dp", "tensor"), None)
    return jax.shard_map(body, mesh=mesh, in_specs=in_specs, out_specs=out_specs, check_vma=False)
```

```python
import functools

import jax
import jax.numpy as jnp
from jax import lax
from jax.experimental import pallas as pl
from jax.experimental.pallas import tpu as pltpu
from jax.sharding import PartitionSpec as P


HEAD_SIZE = 128

epsilon = 1e-05
rope_base = 500000.0
masked = -1e30
initial_peak = -1e29
ROWS = 256
PIECE_SPACE = pltpu.HBM
exp2_scale = 1.4426950408889634 * HEAD_SIZE ** (-0.5)

RING = 4
RELATIVE = (0, 3, 1, 2)


def ring_shift(step):
    return [(i, (i + step) % RING) for i in range(RING)]


def plane_shift(step, first_axis):
    pairs = []
    for d in range(32):
        x, z, core = d // 8, d // 2 % 4, d % 2
        if (core == 0) == first_axis:
            z = (z + step) % 4
        else:
            x = (x + step) % 4
        pairs.append((d, x * 8 + z * 2 + core))
    return pairs


CORE_SWAP = [(d, d ^ 1) for d in range(32)]


def ring_gather(piece, axis, shift):
    half = piece.shape[0] // 2
    behind = lax.ppermute(piece, axis, shift(1))
    ahead = lax.ppermute(piece, axis, shift(-1))
    upper = lax.ppermute(behind[:half], axis, shift(1))
    lower = lax.ppermute(ahead[half:], axis, shift(-1))
    return [piece, behind, ahead, upper, lower]


def gather_plane(keys, values):
    core = lax.axis_index("dp") & 1
    other = lax.ppermute(jnp.where(core == 0, values, keys), "dp", CORE_SWAP)
    mine = jnp.where(
        core == 0,
        jnp.concatenate([keys, other], axis=0),
        jnp.concatenate([other, values], axis=0),
    )
    line = ring_gather(mine, "dp", functools.partial(plane_shift, first_axis=True))
    plane = ring_gather(
        jnp.concatenate(line, axis=0), "dp", functools.partial(plane_shift, first_axis=False)
    )
    return plane, [lax.ppermute(piece, "dp", CORE_SWAP) for piece in plane]


def doc_starts(lengths, positions):
    order = jnp.arange(lengths.shape[0], dtype=jnp.int32)
    doc_ends = jnp.sum(jnp.where(order[:, None] <= order[None, :], lengths[:, None], 0), axis=0)
    closed = (doc_ends[None, :] <= positions[:, None]).astype(jnp.int32)
    return jnp.sum(closed * lengths[None, :], axis=1)


def angles_of(offsets):
    lane = jnp.arange(HEAD_SIZE, dtype=jnp.int32)
    half_width = HEAD_SIZE // 2
    exponent = (lane & (half_width - 1)).astype(jnp.float32) * (-2.0 / HEAD_SIZE)
    frequency = rope_base**exponent
    angles = offsets.astype(jnp.float32)[:, None] * frequency[None, :]
    sign = jnp.where(lane < half_width, -1.0, 1.0).astype(jnp.float32)
    return jnp.cos(angles), jnp.sin(angles) * sign[None, :]


def norm(tokens, norm_gain):
    wide = tokens.astype(jnp.float32)
    inverse = lax.rsqrt(jnp.mean(wide * wide, axis=1, keepdims=True) + epsilon)
    return (wide * inverse * norm_gain[None, :]).astype(jnp.bfloat16)


def wide_dot(a, b):
    return jnp.dot(a, b, preferred_element_type=jnp.float32)


def attend_kernel(ids, lengths, query, cos_part, sin_part, *refs, quarters):
    pieces, refs = refs[:10], refs[10:]
    out, rows, peak, summed, starts, query_at, key_at, block, sems = refs
    own_planes, swapped = pieces[:5], pieces[5:]
    count = query.shape[0]
    heads = query.shape[1] // HEAD_SIZE
    size = block.shape[2]
    span = count // len(quarters)
    docs = lengths.shape[0]
    dp, mine = ids[0], ids[1]
    own_x, own_z, core = dp >> 3, (dp >> 1) & 3, dp & 1

    def quarter_base(quarter):
        return ((mine + RELATIVE[quarter]) & 3) * span

    bases = [dp * (RING * span) + quarter_base(q) for q in quarters]
    first = functools.reduce(jnp.minimum, bases)
    last = functools.reduce(jnp.maximum, bases) + (span - 1)
    ends, end = [], jnp.int32(0)
    for d in range(docs):
        end = end + lengths[d]
        ends.append(end)

    def start_of(at):
        start = jnp.zeros_like(at)
        for end in ends:
            start = jnp.where(at >= end, end, start)
        return start

    first_start, last_start = start_of(first), start_of(last)
    low, high = first_start // size, last // size + 1
    full_low, full_high = (last_start + size - 1) // size, (first + 1) // size

    def place(step):
        return jnp.where(step == 0, 0, jnp.where(step == 1, 2, jnp.where(step == 2, 3, 1)))

    def start_copies(chip):
        slot = chip & 1
        at_x, at_z = place(((chip >> 2) - own_x) & 3), place(((chip & 3) - own_z) & 3)
        outer = jnp.where(core == 0, at_x, at_z)
        inner = jnp.where(core == 0, at_z, at_x)
        for sources, kind, major, minor in (
            (own_planes, core, outer, inner),
            (swapped, 1 - core, inner, outer),
        ):
            index = jnp.where((major == 3) & (minor >= 2), 4, major)
            row = pl.multiple_of(jnp.where(major == 3, minor & 1, minor) * size, size)
            for n, source in enumerate(sources):

                @pl.when(index == n)
                def _():
                    pltpu.make_async_copy(
                        source.at[pl.ds(row, size)], block.at[slot, kind], sems.at[slot, kind]
                    ).start()

    def wait_copies(chip):
        slot = chip & 1
        for kind in range(2):
            pltpu.make_async_copy(
                own_planes[0].at[pl.ds(0, size)], block.at[slot, kind], sems.at[slot, kind]
            ).wait()

    start_copies(low)
    for h in range(heads):
        at = slice(h * HEAD_SIZE, (h + 1) * HEAD_SIZE)
        head = query[:, at]
        turned = head * cos_part[...] + pltpu.roll(head, HEAD_SIZE // 2, 1) * sin_part[...]
        rows[h * count : (h + 1) * count, :] = turned.astype(jnp.bfloat16)
    for i, base in enumerate(bases):
        at = base + lax.broadcasted_iota(jnp.int32, (span, 1), 0)
        query_at[i * span : (i + 1) * span, :] = at
        starts[i * span : (i + 1) * span, :] = start_of(at)
    for i in range(size // span):
        base = (i // RING) * (RING * span) + quarter_base(i % RING)
        lane = lax.broadcasted_iota(jnp.int32, (1, span), 1)
        key_at[:, i * span : (i + 1) * span] = base + lane
    peak[...] = jnp.full(peak.shape, initial_peak, jnp.float32)
    summed[...] = jnp.zeros(summed.shape, jnp.float32)

    def step(chip, cut):
        slot = chip & 1
        block_keys = block[slot, 0]
        block_values = jnp.concatenate(
            [block[slot, 1], jnp.ones((size, HEAD_SIZE), jnp.bfloat16)], axis=1
        )
        if cut:
            where = chip * size + key_at[...]
            visible = (where >= starts[...]) & (where <= query_at[...])
            if count < ROWS:
                visible = jnp.concatenate([visible] * (ROWS // count), axis=0)
        for r in range(heads * count // ROWS):
            at = slice(r * ROWS, (r + 1) * ROWS)
            scores = lax.dot_general(
                rows[at, :], block_keys, (((1,), (1,)), ((), ())), preferred_element_type=jnp.float32
            )
            if cut:
                local = (r * ROWS) % max(count, ROWS)
                scores = jnp.where(visible[local : local + ROWS], scores, masked)
            parts = [scores[:, c : c + HEAD_SIZE] for c in range(0, size, HEAD_SIZE)]
            old = peak[at, :]
            best = functools.reduce(jnp.maximum, parts)
            fresh = jnp.maximum(old, jnp.max(best, axis=1, keepdims=True))
            peak[at, :] = fresh
            shrink = jnp.exp2((old - fresh) * exp2_scale)
            probs = [jnp.exp2((part - fresh) * exp2_scale).astype(jnp.bfloat16) for part in parts]
            update = wide_dot(jnp.concatenate(probs, axis=1), block_values)
            summed[at, :HEAD_SIZE] = summed[at, :HEAD_SIZE] * shrink + update[:, :HEAD_SIZE]
            summed[at, HEAD_SIZE:] = summed[at, HEAD_SIZE:] * shrink + update[:, HEAD_SIZE:]

    def one_block(chip, carry):
        wait_copies(chip)

        @pl.when(chip + 1 < high)
        def _():
            start_copies(chip + 1)

        whole = (chip >= full_low) & (chip < full_high)

        @pl.when(whole)
        def _():
            step(chip, False)

        @pl.when(jnp.logical_not(whole))
        def _():
            step(chip, True)

        return carry

    lax.fori_loop(low, high, one_block, 0)
    for h in range(heads):
        at = slice(h * count, (h + 1) * count)
        attended = summed[at, :HEAD_SIZE] / summed[at, HEAD_SIZE:]
        out[:, h * HEAD_SIZE : (h + 1) * HEAD_SIZE] = attended.astype(jnp.bfloat16)


def attend(ids, lengths, query, cos_part, sin_part, pieces, quarters):
    count, width = query.shape
    rows = count * width // HEAD_SIZE
    size = 2 * RING * count // len(quarters)
    vmem = pl.BlockSpec(memory_space=pltpu.VMEM)
    smem = pl.BlockSpec(memory_space=pltpu.SMEM)
    hbm = pl.BlockSpec(memory_space=PIECE_SPACE)
    return pl.pallas_call(
        functools.partial(attend_kernel, quarters=quarters),
        out_shape=jax.ShapeDtypeStruct((count, width), jnp.bfloat16),
        in_specs=[smem, smem, vmem, vmem, vmem] + [hbm] * 10,
        out_specs=vmem,
        scratch_shapes=[
            pltpu.VMEM((rows, HEAD_SIZE), jnp.bfloat16),
            pltpu.VMEM((rows, HEAD_SIZE), jnp.float32),
            pltpu.VMEM((rows, 2 * HEAD_SIZE), jnp.float32),
            pltpu.VMEM((count, 1), jnp.int32),
            pltpu.VMEM((count, 1), jnp.int32),
            pltpu.VMEM((1, size), jnp.int32),
            pltpu.VMEM((2, 2, size, HEAD_SIZE), jnp.bfloat16),
            pltpu.SemaphoreType.DMA((2, 2)),
        ],
        compiler_params=pltpu.CompilerParams(vmem_limit_bytes=32 * 2**20),
        cost_estimate=pl.CostEstimate(
            flops=rows * 4096 * 512, transcendentals=rows * 4096, bytes_accessed=4 << 20
        ),
        name="attend",
    )(ids, lengths, query, cos_part, sin_part, *pieces)


def body(tokens, norm_gain, w_query, key_weight, value_weight, w_out, lengths):
    count = tokens.shape[0]
    dp, mine = lax.axis_index("dp"), lax.axis_index("tensor")
    normed = norm(tokens, norm_gain)
    quarter = (mine + jnp.array(RELATIVE, jnp.int32)) & 3
    local = (quarter[:, None] * count + jnp.arange(count, dtype=jnp.int32)[None, :]).reshape(-1)
    positions = dp * (RING * count) + local
    cos_part, sin_part = angles_of(positions - doc_starts(lengths, positions))
    ids = jnp.stack([dp, mine]).astype(jnp.int32)

    def project(piece, q):
        at = slice(q * count, (q + 1) * count)
        key = wide_dot(piece, key_weight)
        key = key * cos_part[at] + jnp.roll(key, HEAD_SIZE // 2, axis=1) * sin_part[at]
        value = wide_dot(piece, value_weight)
        return key.astype(jnp.bfloat16), value.astype(jnp.bfloat16)

    own = normed
    behind = lax.ppermute(own, "tensor", ring_shift(1))
    ahead = lax.ppermute(own, "tensor", ring_shift(-1))
    query = [None] * RING
    keys, values = [None] * RING, [None] * RING
    keys[0], values[0] = project(own, 0)
    query[0] = wide_dot(own, w_query)
    behind, ahead, query[0], keys[0], values[0] = lax.optimization_barrier(
        (behind, ahead, query[0], keys[0], values[0])
    )
    half = count // 2
    upper = lax.ppermute(behind[:half], "tensor", ring_shift(1))
    lower = lax.ppermute(ahead[half:], "tensor", ring_shift(-1))
    keys[1], values[1] = project(behind, 1)
    keys[2], values[2] = project(ahead, 2)
    query[1] = wide_dot(behind, w_query)
    query[2] = wide_dot(ahead, w_query)
    upper, lower, query[1], query[2], keys[1], values[1], keys[2], values[2] = (
        lax.optimization_barrier(
            (upper, lower, query[1], query[2], keys[1], values[1], keys[2], values[2])
        )
    )
    far = jnp.concatenate([upper, lower], axis=0)
    keys[3], values[3] = project(far, 3)
    pieces = gather_plane(jnp.concatenate(keys, axis=0), jnp.concatenate(values, axis=0))
    query[3] = wide_dot(far, w_query)
    plane, swapped = pieces
    pieces = list(plane) + list(swapped)

    def branch(quarters, after=None):
        at = slice(quarters[0] * count, (quarters[-1] + 1) * count)
        rows = jnp.concatenate([query[q] for q in quarters], axis=0)
        if after is not None:
            rows, after = lax.optimization_barrier((rows, after))
        attended = attend(ids, lengths, rows, cos_part[at], sin_part[at], pieces, quarters)
        return wide_dot(attended, w_out), after

    half = w_out.shape[1] // 2
    far, _ = branch((3,))
    far = far.astype(jnp.bfloat16)
    near, far = branch((1, 2), far)
    from_behind = lax.ppermute(far[:, :half], "tensor", ring_shift(1))
    from_ahead = lax.ppermute(far[:, half:], "tensor", ring_shift(-1))
    to_behind, to_ahead = near[:count], near[count:]
    plain_up = to_ahead[:, half:].astype(jnp.bfloat16)
    plain_up = lax.ppermute(plain_up, "tensor", ring_shift(1))
    plain_down = to_behind[:, :half].astype(jnp.bfloat16)
    plain_down = lax.ppermute(plain_down, "tensor", ring_shift(-1))
    sum_up = (to_ahead[:, :half] + from_behind.astype(jnp.float32)).astype(jnp.bfloat16)
    sum_down = (to_behind[:, half:] + from_ahead.astype(jnp.float32)).astype(jnp.bfloat16)
    here, (sum_up, sum_down) = branch((0,), (sum_up, sum_down))
    sum_up = lax.ppermute(sum_up, "tensor", ring_shift(1))
    sum_down = lax.ppermute(sum_down, "tensor", ring_shift(-1))
    wide = [a.astype(jnp.float32) for a in (sum_up, plain_down, plain_up, sum_down)]
    total = here + jnp.concatenate([wide[0] + wide[1], wide[2] + wide[3]], axis=1)
    return (tokens.astype(jnp.float32) + total).astype(jnp.bfloat16)


def solution(mesh):
    in_specs = (
        P(("dp", "tensor"), None),
        P(),
        P(None, "tensor"),
        P(None, "tensor"),
        P(None, "tensor"),
        P("tensor", None),
        P(),
    )
    out_specs = P(("dp", "tensor"), None)
    return jax.shard_map(body, mesh=mesh, in_specs=in_specs, out_specs=out_specs, check_vma=False)
```

```python
import functools

import jax
import jax.numpy as jnp
from jax import lax
from jax.experimental import pallas as pl
from jax.experimental.pallas import tpu as pltpu
from jax.sharding import PartitionSpec as P


HEAD_SIZE = 128

epsilon = 1e-05
rope_base = 500000.0
masked = -1e30
initial_peak = -1e29
ROWS = 256
PIECE_SPACE = pltpu.HBM
exp2_scale = 1.4426950408889634 * HEAD_SIZE ** (-0.5)

RING = 4
RELATIVE = (0, 3, 1, 2)
KEY_ORDER = ((0, 0), (0, 1), (0, 2), (1, 0), (1, 1), (1, 2), (0, 3), (1, 3))


def ring_shift(step):
    return [(i, (i + step) % RING) for i in range(RING)]


def plane_shift(step, first_axis):
    pairs = []
    for d in range(32):
        x, z, core = d // 8, d // 2 % 4, d % 2
        if (core == 0) == first_axis:
            z = (z + step) % 4
        else:
            x = (x + step) % 4
        pairs.append((d, x * 8 + z * 2 + core))
    return pairs


CORE_SWAP = [(d, d ^ 1) for d in range(32)]


def ring_gather(piece, axis, shift):
    half = piece.shape[0] // 2
    behind = lax.ppermute(piece, axis, shift(1))
    ahead = lax.ppermute(piece, axis, shift(-1))
    upper = lax.ppermute(behind[:half], axis, shift(1))
    lower = lax.ppermute(ahead[half:], axis, shift(-1))
    return [piece, behind, ahead, upper, lower]


def gather_plane(keys, values):
    core = lax.axis_index("dp") & 1
    other = lax.ppermute(jnp.where(core == 0, values, keys), "dp", CORE_SWAP)
    mine = jnp.where(
        core == 0,
        jnp.concatenate([keys, other], axis=0),
        jnp.concatenate([other, values], axis=0),
    )
    shift = functools.partial(plane_shift, first_axis=True)
    line = ring_gather(mine, "dp", shift)
    shift = functools.partial(plane_shift, first_axis=False)
    plane = ring_gather(jnp.concatenate(line, axis=0), "dp", shift)
    return plane + [lax.ppermute(piece, "dp", CORE_SWAP) for piece in plane]


def doc_starts(lengths, positions):
    order = jnp.arange(lengths.shape[0], dtype=jnp.int32)
    doc_ends = jnp.sum(jnp.where(order[:, None] <= order[None, :], lengths[:, None], 0), axis=0)
    closed = (doc_ends[None, :] <= positions[:, None]).astype(jnp.int32)
    return jnp.sum(closed * lengths[None, :], axis=1)


def angles_of(offsets):
    lane = jnp.arange(HEAD_SIZE, dtype=jnp.int32)
    half_width = HEAD_SIZE // 2
    exponent = (lane & (half_width - 1)).astype(jnp.float32) * (-2.0 / HEAD_SIZE)
    frequency = rope_base**exponent
    angles = offsets.astype(jnp.float32)[:, None] * frequency[None, :]
    sign = jnp.where(lane < half_width, -1.0, 1.0).astype(jnp.float32)
    return jnp.cos(angles), jnp.sin(angles) * sign[None, :]


def norm(tokens, norm_gain):
    wide = tokens.astype(jnp.float32)
    inverse = lax.rsqrt(jnp.mean(wide * wide, axis=1, keepdims=True) + epsilon)
    return (wide * inverse * norm_gain[None, :]).astype(jnp.bfloat16)


def wide_dot(a, b):
    return jnp.dot(a, b, preferred_element_type=jnp.float32)


def attend_kernel(ids, lengths, query, cos_part, sin_part, *refs, quarters):
    bulk, rest, refs = refs[:10], refs[10:20], refs[20:]
    out, rows, peak, summed, starts, query_at, key_at, block, sems = refs
    count = query.shape[0]
    heads = query.shape[1] // HEAD_SIZE
    size = block.shape[2]
    span = count // len(quarters)
    docs = lengths.shape[0]
    dp, mine = ids[0], ids[1]
    own_x, own_z, core = dp >> 3, (dp >> 1) & 3, dp & 1

    def quarter_base(quarter):
        return ((mine + RELATIVE[quarter]) & 3) * span

    bases = [dp * (RING * span) + quarter_base(q) for q in quarters]
    first = functools.reduce(jnp.minimum, bases)
    last = functools.reduce(jnp.maximum, bases) + (span - 1)
    ends, end = [], jnp.int32(0)
    for d in range(docs):
        end = end + lengths[d]
        ends.append(end)

    def start_of(at):
        start = jnp.zeros_like(at)
        for end in ends:
            start = jnp.where(at >= end, end, start)
        return start

    first_start, last_start = start_of(first), start_of(last)
    low, high = first_start // size, last // size + 1
    full_low, full_high = (last_start + size - 1) // size, (first + 1) // size

    def place(step):
        return jnp.where(step == 0, 0, jnp.where(step == 1, 2, jnp.where(step == 2, 3, 1)))

    def start_copies(chip):
        slot = chip & 1
        at_x, at_z = place(((chip >> 2) - own_x) & 3), place(((chip & 3) - own_z) & 3)
        outer = jnp.where(core == 0, at_x, at_z)
        inner = jnp.where(core == 0, at_z, at_x)
        for side, kind, major, minor in ((0, core, outer, inner), (5, 1 - core, inner, outer)):
            index = jnp.where((major == 3) & (minor >= 2), 4, major)
            line = jnp.where(major == 3, minor & 1, minor)
            for n in range(5):

                @pl.when(index == n)
                def _():
                    for sources, at, length in ((bulk, 0, 6 * span), (rest, 6 * span, 2 * span)):
                        pltpu.make_async_copy(
                            sources[side + n].at[pl.ds(pl.multiple_of(line * length, length), length)],
                            block.at[slot, kind, at : at + length],
                            sems.at[slot, kind],
                        ).start()

    def wait_copies(chip):
        slot = chip & 1
        for kind in range(2):
            pltpu.make_async_copy(
                bulk[0].at[pl.ds(0, size)], block.at[slot, kind], sems.at[slot, kind]
            ).wait()

    start_copies(low)
    for h in range(heads):
        at = slice(h * HEAD_SIZE, (h + 1) * HEAD_SIZE)
        head = query[:, at]
        turned = head * cos_part[...] + pltpu.roll(head, HEAD_SIZE // 2, 1) * sin_part[...]
        rows[h * count : (h + 1) * count, :] = turned.astype(jnp.bfloat16)
    for i, base in enumerate(bases):
        at = base + lax.broadcasted_iota(jnp.int32, (span, 1), 0)
        query_at[i * span : (i + 1) * span, :] = at
        starts[i * span : (i + 1) * span, :] = start_of(at)
    for i, (half, quarter) in enumerate(KEY_ORDER):
        base = half * (RING * span) + quarter_base(quarter)
        lane = lax.broadcasted_iota(jnp.int32, (1, span), 1)
        key_at[:, i * span : (i + 1) * span] = base + lane
    peak[...] = jnp.full(peak.shape, initial_peak, jnp.float32)
    summed[...] = jnp.zeros(summed.shape, jnp.float32)

    def step(chip, cut):
        slot = chip & 1
        block_keys = block[slot, 0]
        block_values = jnp.concatenate(
            [block[slot, 1], jnp.ones((size, HEAD_SIZE), jnp.bfloat16)], axis=1
        )
        if cut:
            where = chip * size + key_at[...]
            visible = (where >= starts[...]) & (where <= query_at[...])
            if count < ROWS:
                visible = jnp.concatenate([visible] * (ROWS // count), axis=0)
        for r in range(heads * count // ROWS):
            at = slice(r * ROWS, (r + 1) * ROWS)
            scores = lax.dot_general(
                rows[at, :], block_keys, (((1,), (1,)), ((), ())), preferred_element_type=jnp.float32
            )
            if cut:
                local = (r * ROWS) % max(count, ROWS)
                scores = jnp.where(visible[local : local + ROWS], scores, masked)
            parts = [scores[:, c : c + HEAD_SIZE] for c in range(0, size, HEAD_SIZE)]
            old = peak[at, :]
            best = functools.reduce(jnp.maximum, parts)
            fresh = jnp.maximum(old, jnp.max(best, axis=1, keepdims=True))
            peak[at, :] = fresh
            shrink = jnp.exp2((old - fresh) * exp2_scale)
            probs = [jnp.exp2((part - fresh) * exp2_scale).astype(jnp.bfloat16) for part in parts]
            update = wide_dot(jnp.concatenate(probs, axis=1), block_values)
            summed[at, :HEAD_SIZE] = summed[at, :HEAD_SIZE] * shrink + update[:, :HEAD_SIZE]
            summed[at, HEAD_SIZE:] = summed[at, HEAD_SIZE:] * shrink + update[:, HEAD_SIZE:]

    def one_block(chip, carry):
        wait_copies(chip)

        @pl.when(chip + 1 < high)
        def _():
            start_copies(chip + 1)

        whole = (chip >= full_low) & (chip < full_high)

        @pl.when(whole)
        def _():
            step(chip, False)

        @pl.when(jnp.logical_not(whole))
        def _():
            step(chip, True)

        return carry

    lax.fori_loop(low, high, one_block, 0)
    for h in range(heads):
        at = slice(h * count, (h + 1) * count)
        attended = summed[at, :HEAD_SIZE] / summed[at, HEAD_SIZE:]
        out[:, h * HEAD_SIZE : (h + 1) * HEAD_SIZE] = attended.astype(jnp.bfloat16)


def attend(ids, lengths, query, cos_part, sin_part, pieces, quarters):
    count, width = query.shape
    rows = count * width // HEAD_SIZE
    size = 2 * RING * count // len(quarters)
    vmem = pl.BlockSpec(memory_space=pltpu.VMEM)
    smem = pl.BlockSpec(memory_space=pltpu.SMEM)
    hbm = pl.BlockSpec(memory_space=PIECE_SPACE)
    return pl.pallas_call(
        functools.partial(attend_kernel, quarters=quarters),
        out_shape=jax.ShapeDtypeStruct((count, width), jnp.bfloat16),
        in_specs=[smem, smem, vmem, vmem, vmem] + [hbm] * 20,
        out_specs=vmem,
        scratch_shapes=[
            pltpu.VMEM((rows, HEAD_SIZE), jnp.bfloat16),
            pltpu.VMEM((rows, HEAD_SIZE), jnp.float32),
            pltpu.VMEM((rows, 2 * HEAD_SIZE), jnp.float32),
            pltpu.VMEM((count, 1), jnp.int32),
            pltpu.VMEM((count, 1), jnp.int32),
            pltpu.VMEM((1, size), jnp.int32),
            pltpu.VMEM((2, 2, size, HEAD_SIZE), jnp.bfloat16),
            pltpu.SemaphoreType.DMA((2, 2)),
        ],
        compiler_params=pltpu.CompilerParams(vmem_limit_bytes=56 * 2**20),
        cost_estimate=pl.CostEstimate(
            flops=rows * 4096 * 512, transcendentals=rows * 4096, bytes_accessed=4 << 20
        ),
        name="attend",
    )(ids, lengths, query, cos_part, sin_part, *pieces)


def body(tokens, norm_gain, w_query, key_weight, value_weight, w_out, lengths):
    count = tokens.shape[0]
    dp, mine = lax.axis_index("dp"), lax.axis_index("tensor")
    normed = norm(tokens, norm_gain)
    quarter = (mine + jnp.array(RELATIVE, jnp.int32)) & 3
    local = (quarter[:, None] * count + jnp.arange(count, dtype=jnp.int32)[None, :]).reshape(-1)
    positions = dp * (RING * count) + local
    cos_part, sin_part = angles_of(positions - doc_starts(lengths, positions))
    ids = jnp.stack([dp, mine]).astype(jnp.int32)

    def project(piece, q):
        at = slice(q * count, (q + 1) * count)
        key = wide_dot(piece, key_weight)
        key = key * cos_part[at] + jnp.roll(key, HEAD_SIZE // 2, axis=1) * sin_part[at]
        value = wide_dot(piece, value_weight)
        return key.astype(jnp.bfloat16), value.astype(jnp.bfloat16)

    half = count // 2
    query = [None] * RING
    keys, values = [None] * RING, [None] * RING
    keys[0], values[0] = project(normed, 0)
    query[0] = wide_dot(normed, w_query)
    behind_top = lax.ppermute(normed[:half], "tensor", ring_shift(1))
    ahead_low = lax.ppermute(normed[half:], "tensor", ring_shift(-1))
    behind_low = lax.ppermute(normed[half:], "tensor", ring_shift(1))
    ahead_top = lax.ppermute(normed[:half], "tensor", ring_shift(-1))
    far_top = lax.ppermute(behind_top, "tensor", ring_shift(1))
    far_low = lax.ppermute(ahead_low, "tensor", ring_shift(-1))
    behind_low, ahead_top, query[0], keys[0], values[0] = lax.optimization_barrier(
        (behind_low, ahead_top, query[0], keys[0], values[0])
    )
    behind = jnp.concatenate([behind_top, behind_low], axis=0)
    ahead = jnp.concatenate([ahead_top, ahead_low], axis=0)
    keys[1], values[1] = project(behind, 1)
    keys[2], values[2] = project(ahead, 2)
    query[1] = wide_dot(behind, w_query)
    query[2] = wide_dot(ahead, w_query)
    bulk = gather_plane(jnp.concatenate(keys[:3], axis=0), jnp.concatenate(values[:3], axis=0))
    far_top, far_low, query[1], query[2] = lax.optimization_barrier(
        (far_top, far_low, query[1], query[2])
    )
    far = jnp.concatenate([far_top, far_low], axis=0)
    keys[3], values[3] = project(far, 3)
    rest = gather_plane(keys[3], values[3])
    query[3] = wide_dot(far, w_query)
    pieces = bulk + rest

    def branch(quarters, after=None):
        at = slice(quarters[0] * count, (quarters[-1] + 1) * count)
        rows = jnp.concatenate([query[q] for q in quarters], axis=0)
        if after is not None:
            rows, after = lax.optimization_barrier((rows, after))
        attended = attend(ids, lengths, rows, cos_part[at], sin_part[at], pieces, quarters)
        return wide_dot(attended, w_out), after

    half = w_out.shape[1] // 2
    far, _ = branch((3,))
    far = far.astype(jnp.bfloat16)
    near, far = branch((1, 2), far)
    from_behind = lax.ppermute(far[:, :half], "tensor", ring_shift(1))
    from_ahead = lax.ppermute(far[:, half:], "tensor", ring_shift(-1))
    to_behind, to_ahead = near[:count], near[count:]
    plain_up = to_ahead[:, half:].astype(jnp.bfloat16)
    plain_up = lax.ppermute(plain_up, "tensor", ring_shift(1))
    plain_down = to_behind[:, :half].astype(jnp.bfloat16)
    plain_down = lax.ppermute(plain_down, "tensor", ring_shift(-1))
    sum_up = (to_ahead[:, :half] + from_behind.astype(jnp.float32)).astype(jnp.bfloat16)
    sum_down = (to_behind[:, half:] + from_ahead.astype(jnp.float32)).astype(jnp.bfloat16)
    here, (sum_up, sum_down) = branch((0,), (sum_up, sum_down))
    sum_up = lax.ppermute(sum_up, "tensor", ring_shift(1))
    sum_down = lax.ppermute(sum_down, "tensor", ring_shift(-1))
    wide = [a.astype(jnp.float32) for a in (sum_up, plain_down, plain_up, sum_down)]
    total = here + jnp.concatenate([wide[0] + wide[1], wide[2] + wide[3]], axis=1)
    return (tokens.astype(jnp.float32) + total).astype(jnp.bfloat16)


def solution(mesh):
    in_specs = (
        P(("dp", "tensor"), None),
        P(),
        P(None, "tensor"),
        P(None, "tensor"),
        P(None, "tensor"),
        P("tensor", None),
        P(),
    )
    out_specs = P(("dp", "tensor"), None)
    return jax.shard_map(body, mesh=mesh, in_specs=in_specs, out_specs=out_specs, check_vma=False)
```

```python
import functools

import jax
import jax.numpy as jnp
from jax import lax
from jax.experimental import pallas as pl
from jax.experimental.pallas import tpu as pltpu
from jax.sharding import PartitionSpec as P


HEAD_SIZE = 128

epsilon = 1e-05
rope_base = 500000.0
masked = -1e30
initial_peak = -1e29
ROWS = 256
SLOTS = 4
PIECE_SPACE = pltpu.HBM
exp2_scale = 1.4426950408889634 * HEAD_SIZE ** (-0.5)

RING = 4
RELATIVE = (0, 3, 1, 2)
KEY_ORDER = ((0, 0), (0, 1), (0, 2), (1, 0), (1, 1), (1, 2), (0, 3), (1, 3))


def ring_shift(step):
    return [(i, (i + step) % RING) for i in range(RING)]


def plane_shift(step, first_axis):
    pairs = []
    for d in range(32):
        x, z, core = d // 8, d // 2 % 4, d % 2
        if (core == 0) == first_axis:
            z = (z + step) % 4
        else:
            x = (x + step) % 4
        pairs.append((d, x * 8 + z * 2 + core))
    return pairs


CORE_SWAP = [(d, d ^ 1) for d in range(32)]


def ring_gather(piece, axis, shift):
    half = piece.shape[0] // 2
    behind = lax.ppermute(piece, axis, shift(1))
    ahead = lax.ppermute(piece, axis, shift(-1))
    upper = lax.ppermute(behind[:half], axis, shift(1))
    lower = lax.ppermute(ahead[half:], axis, shift(-1))
    return [piece, behind, ahead, upper, lower]


def gather_plane(keys, values, whole):
    core = lax.axis_index("dp") & 1
    other = lax.ppermute(jnp.where(core == 0, values, keys), "dp", CORE_SWAP)
    mine = jnp.where(
        core == 0,
        jnp.concatenate([keys, other], axis=0),
        jnp.concatenate([other, values], axis=0),
    )
    shift = functools.partial(plane_shift, first_axis=True)
    line = ring_gather(mine, "dp", shift)
    shift = functools.partial(plane_shift, first_axis=False)
    plane = ring_gather(jnp.concatenate(line, axis=0), "dp", shift)
    if whole:
        plane = [jnp.concatenate(plane, axis=0)]
    traded = [lax.ppermute(piece, "dp", CORE_SWAP) for piece in plane[:3]]
    traded += [lax.ppermute(piece, "dp", CORE_SWAP) for piece in plane[3:]]
    return plane + traded


def doc_starts(lengths, positions):
    order = jnp.arange(lengths.shape[0], dtype=jnp.int32)
    doc_ends = jnp.sum(jnp.where(order[:, None] <= order[None, :], lengths[:, None], 0), axis=0)
    closed = (doc_ends[None, :] <= positions[:, None]).astype(jnp.int32)
    return jnp.sum(closed * lengths[None, :], axis=1)


def angles_of(offsets):
    lane = jnp.arange(HEAD_SIZE, dtype=jnp.int32)
    half_width = HEAD_SIZE // 2
    exponent = (lane & (half_width - 1)).astype(jnp.float32) * (-2.0 / HEAD_SIZE)
    frequency = rope_base**exponent
    angles = offsets.astype(jnp.float32)[:, None] * frequency[None, :]
    sign = jnp.where(lane < half_width, -1.0, 1.0).astype(jnp.float32)
    return jnp.cos(angles), jnp.sin(angles) * sign[None, :]


def norm(tokens, norm_gain):
    wide = tokens.astype(jnp.float32)
    inverse = lax.rsqrt(jnp.mean(wide * wide, axis=1, keepdims=True) + epsilon)
    return (wide * inverse * norm_gain[None, :]).astype(jnp.bfloat16)


def wide_dot(a, b):
    return jnp.dot(a, b, preferred_element_type=jnp.float32)


def attend_kernel(ids, lengths, query, cos_part, sin_part, *refs, quarters):
    bulk, rest, refs = refs[:10], refs[10:12], refs[12:]
    out, rows, scores, peak, summed, starts, query_at, key_at, block, sems = refs
    count = query.shape[0]
    heads = query.shape[1] // HEAD_SIZE
    size = block.shape[2]
    span = count // len(quarters)
    docs = lengths.shape[0]
    dp, mine = ids[0], ids[1]
    own_x, own_z, core = dp >> 3, (dp >> 1) & 3, dp & 1

    def quarter_base(quarter):
        return ((mine + RELATIVE[quarter]) & 3) * span

    bases = [dp * (RING * span) + quarter_base(q) for q in quarters]
    first = functools.reduce(jnp.minimum, bases)
    last = functools.reduce(jnp.maximum, bases) + (span - 1)
    ends, end = [], jnp.int32(0)
    for d in range(docs):
        end = end + lengths[d]
        ends.append(end)

    def start_of(at):
        start = jnp.zeros_like(at)
        for end in ends:
            start = jnp.where(at >= end, end, start)
        return start

    first_start, last_start = start_of(first), start_of(last)
    low, high = first_start // size, last // size + 1
    full_low, full_high = (last_start + size - 1) // size, (first + 1) // size

    most, few = 6 * span, 2 * span

    def place(step):
        return jnp.where(step == 0, 0, jnp.where(step == 1, 2, jnp.where(step == 2, 3, 1)))

    def start_copies(chip):
        slot = chip & (SLOTS - 1)
        at_x, at_z = place(((chip >> 2) - own_x) & 3), place(((chip & 3) - own_z) & 3)
        outer = jnp.where(core == 0, at_x, at_z)
        inner = jnp.where(core == 0, at_z, at_x)
        for side, kind, major, minor in ((0, core, outer, inner), (5, 1 - core, inner, outer)):
            index = jnp.where((major == 3) & (minor >= 2), 4, major)
            line = jnp.where(major == 3, minor & 1, minor)
            for n in range(5):

                @pl.when(index == n)
                def _():
                    pltpu.make_async_copy(
                        bulk[side + n].at[pl.ds(pl.multiple_of(line * most, most), most)],
                        block.at[slot, kind, :most],
                        sems.at[slot, kind],
                    ).start()

            pltpu.make_async_copy(
                rest[side // 5].at[
                    pl.ds(pl.multiple_of((RING * major + minor) * few, few), few)
                ],
                block.at[slot, kind, most:],
                sems.at[slot, kind],
            ).start()

    def wait_copies(chip):
        slot = chip & (SLOTS - 1)
        for kind in range(2):
            pltpu.make_async_copy(
                bulk[0].at[pl.ds(0, size)], block.at[slot, kind], sems.at[slot, kind]
            ).wait()

    def begin(chip, carry):
        start_copies(chip)
        return carry

    lax.fori_loop(low, jnp.minimum(low + (SLOTS - 1), high), begin, 0)
    here = slice(quarters[0] * span, quarters[0] * span + count)
    for h in range(heads):
        at = slice(h * HEAD_SIZE, (h + 1) * HEAD_SIZE)
        head = query[:, at]
        turned = head * cos_part[here, :] + pltpu.roll(head, HEAD_SIZE // 2, 1) * sin_part[here, :]
        rows[h * count : (h + 1) * count, :] = turned.astype(jnp.bfloat16)
    for i, base in enumerate(bases):
        at = base + lax.broadcasted_iota(jnp.int32, (span, 1), 0)
        query_at[i * span : (i + 1) * span, :] = at
        starts[i * span : (i + 1) * span, :] = start_of(at)
    for i, (half, quarter) in enumerate(KEY_ORDER):
        base = half * (RING * span) + quarter_base(quarter)
        lane = lax.broadcasted_iota(jnp.int32, (1, span), 1)
        key_at[:, i * span : (i + 1) * span] = base + lane
    peak[...] = jnp.full(peak.shape, initial_peak, jnp.float32)
    summed[...] = jnp.zeros(summed.shape, jnp.float32)

    def score(chip, at):
        scores[at, :] = lax.dot_general(
            rows[at, :],
            block[chip & (SLOTS - 1), 0],
            (((1,), (1,)), ((), ())),
            preferred_element_type=jnp.float32,
        )

    def step(chip, cut):
        slot = chip & (SLOTS - 1)
        block_values = jnp.concatenate(
            [block[slot, 1], jnp.ones((size, HEAD_SIZE), jnp.bfloat16)], axis=1
        )
        if cut:
            where = chip * size + key_at[...]
            scores_seen = (where >= starts[...]) & (where <= query_at[...])
            if count < ROWS:
                scores_seen = jnp.concatenate([scores_seen] * (ROWS // count), axis=0)
        for r in range(heads * count // ROWS):
            at = slice(r * ROWS, (r + 1) * ROWS)
            local = (r * ROWS) % max(count, ROWS)

            def part(c):
                here = scores[at, c : c + HEAD_SIZE]
                if cut:
                    here = jnp.where(
                        scores_seen[local : local + ROWS, c : c + HEAD_SIZE], here, masked
                    )
                return here

            old = peak[at, :]
            columns = range(0, size, HEAD_SIZE)
            best = functools.reduce(jnp.maximum, [part(c) for c in columns])
            fresh = jnp.maximum(old, jnp.max(best, axis=1, keepdims=True))
            peak[at, :] = fresh
            shrink = jnp.exp2((old - fresh) * exp2_scale)
            probs = [jnp.exp2((part(c) - fresh) * exp2_scale).astype(jnp.bfloat16) for c in columns]
            update = wide_dot(jnp.concatenate(probs, axis=1), block_values)
            summed[at, :HEAD_SIZE] = summed[at, :HEAD_SIZE] * shrink + update[:, :HEAD_SIZE]
            summed[at, HEAD_SIZE:] = summed[at, HEAD_SIZE:] * shrink + update[:, HEAD_SIZE:]
            score(chip + 1, at)

    def one_block(chip, carry):
        @pl.when(chip + 1 < high)
        def _():
            wait_copies(chip + 1)

        @pl.when(chip + (SLOTS - 1) < high)
        def _():
            start_copies(chip + (SLOTS - 1))

        whole = (chip >= full_low) & (chip < full_high)

        @pl.when(whole)
        def _():
            step(chip, False)

        @pl.when(jnp.logical_not(whole))
        def _():
            step(chip, True)

        return carry

    wait_copies(low)
    for r in range(heads * count // ROWS):
        score(low, slice(r * ROWS, (r + 1) * ROWS))
    lax.fori_loop(low, high, one_block, 0)
    for h in range(heads):
        at = slice(h * count, (h + 1) * count)
        attended = summed[at, :HEAD_SIZE] / summed[at, HEAD_SIZE:]
        out[:, h * HEAD_SIZE : (h + 1) * HEAD_SIZE] = attended.astype(jnp.bfloat16)


def attend(ids, lengths, query, cos_part, sin_part, pieces, quarters):
    count, width = query.shape
    rows = count * width // HEAD_SIZE
    size = 2 * RING * count // len(quarters)
    vmem = pl.BlockSpec(memory_space=pltpu.VMEM)
    smem = pl.BlockSpec(memory_space=pltpu.SMEM)
    hbm = pl.BlockSpec(memory_space=PIECE_SPACE)
    return pl.pallas_call(
        functools.partial(attend_kernel, quarters=quarters),
        out_shape=jax.ShapeDtypeStruct((count, width), jnp.bfloat16),
        in_specs=[smem, smem, vmem, vmem, vmem] + [hbm] * 12,
        out_specs=vmem,
        scratch_shapes=[
            pltpu.VMEM((rows, HEAD_SIZE), jnp.bfloat16),
            pltpu.VMEM((rows, size), jnp.float32),
            pltpu.VMEM((rows, HEAD_SIZE), jnp.float32),
            pltpu.VMEM((rows, 2 * HEAD_SIZE), jnp.float32),
            pltpu.VMEM((count, 1), jnp.int32),
            pltpu.VMEM((count, 1), jnp.int32),
            pltpu.VMEM((1, size), jnp.int32),
            pltpu.VMEM((SLOTS, 2, size, HEAD_SIZE), jnp.bfloat16),
            pltpu.SemaphoreType.DMA((SLOTS, 2)),
        ],
        compiler_params=pltpu.CompilerParams(vmem_limit_bytes=56 * 2**20),
        cost_estimate=pl.CostEstimate(
            flops=rows * 4096 * 512, transcendentals=rows * 4096, bytes_accessed=4 << 20
        ),
        name="attend",
    )(ids, lengths, query, cos_part, sin_part, *pieces)


def body(tokens, norm_gain, w_query, key_weight, value_weight, w_out, lengths):
    count = tokens.shape[0]
    dp, mine = lax.axis_index("dp"), lax.axis_index("tensor")
    normed = norm(tokens, norm_gain)
    quarter = (mine + jnp.array(RELATIVE, jnp.int32)) & 3
    local = (quarter[:, None] * count + jnp.arange(count, dtype=jnp.int32)[None, :]).reshape(-1)
    positions = dp * (RING * count) + local
    cos_part, sin_part = angles_of(positions - doc_starts(lengths, positions))
    ids = jnp.stack([dp, mine]).astype(jnp.int32)

    def project(piece, first):
        at = slice(first, first + piece.shape[0])
        key = wide_dot(piece, key_weight)
        key = key * cos_part[at] + jnp.roll(key, HEAD_SIZE // 2, axis=1) * sin_part[at]
        value = wide_dot(piece, value_weight)
        return key.astype(jnp.bfloat16), value.astype(jnp.bfloat16)

    half = count // 2
    query = [None] * RING
    kv_own = project(normed, 0)
    query[0] = wide_dot(normed, w_query)
    behind_top = lax.ppermute(normed[:half], "tensor", ring_shift(1))
    ahead_low = lax.ppermute(normed[half:], "tensor", ring_shift(-1))
    behind_low = lax.ppermute(normed[half:], "tensor", ring_shift(1))
    ahead_top = lax.ppermute(normed[:half], "tensor", ring_shift(-1))
    far_top = lax.ppermute(behind_top, "tensor", ring_shift(1))
    far_low = lax.ppermute(ahead_low, "tensor", ring_shift(-1))
    kv_behind_top = project(behind_top, count)
    kv_ahead_low = project(ahead_low, 2 * count + half)
    behind_low, ahead_top, query[0], kv_own, kv_behind_top, kv_ahead_low, ids = (
        lax.optimization_barrier(
            (behind_low, ahead_top, query[0], kv_own, kv_behind_top, kv_ahead_low, ids)
        )
    )
    kv_behind_low = project(behind_low, count + half)
    kv_ahead_top = project(ahead_top, 2 * count)
    near = [wide_dot(a, w_query) for a in (behind_top, behind_low, ahead_top, ahead_low)]
    kv_near = (kv_own, kv_behind_top, kv_behind_low, kv_ahead_top, kv_ahead_low)
    bulk = gather_plane(*[jnp.concatenate(a, axis=0) for a in zip(*kv_near)], False)
    far_top, far_low, near = lax.optimization_barrier((far_top, far_low, near))
    far = jnp.concatenate([far_top, far_low], axis=0)
    rest = gather_plane(*project(far, 3 * count), True)
    query[3] = wide_dot(far, w_query)
    near_rows = jnp.concatenate(near, axis=0)
    pieces = bulk + rest

    def branch(quarters, after=None):
        rows = near_rows if len(quarters) == 2 else query[quarters[0]]
        if after is not None:
            rows, after = lax.optimization_barrier((rows, after))
        attended = attend(ids, lengths, rows, cos_part, sin_part, pieces, quarters)
        return wide_dot(attended, w_out), after

    half = w_out.shape[1] // 2
    far, _ = branch((3,))
    far = far.astype(jnp.bfloat16)
    near, far = branch((1, 2), far)
    from_behind = lax.ppermute(far[:, :half], "tensor", ring_shift(1))
    from_ahead = lax.ppermute(far[:, half:], "tensor", ring_shift(-1))
    to_behind, to_ahead = near[:count], near[count:]
    plain_up = to_ahead[:, half:].astype(jnp.bfloat16)
    plain_up = lax.ppermute(plain_up, "tensor", ring_shift(1))
    plain_down = to_behind[:, :half].astype(jnp.bfloat16)
    plain_down = lax.ppermute(plain_down, "tensor", ring_shift(-1))
    sum_up = (to_ahead[:, :half] + from_behind.astype(jnp.float32)).astype(jnp.bfloat16)
    sum_down = (to_behind[:, half:] + from_ahead.astype(jnp.float32)).astype(jnp.bfloat16)
    here, (sum_up, sum_down) = branch((0,), (sum_up, sum_down))
    sum_up = lax.ppermute(sum_up, "tensor", ring_shift(1))
    sum_down = lax.ppermute(sum_down, "tensor", ring_shift(-1))
    wide = [a.astype(jnp.float32) for a in (sum_up, plain_down, plain_up, sum_down)]
    total = here + jnp.concatenate([wide[0] + wide[1], wide[2] + wide[3]], axis=1)
    return (tokens.astype(jnp.float32) + total).astype(jnp.bfloat16)


def solution(mesh):
    in_specs = (
        P(("dp", "tensor"), None),
        P(),
        P(None, "tensor"),
        P(None, "tensor"),
        P(None, "tensor"),
        P("tensor", None),
        P(),
    )
    out_specs = P(("dp", "tensor"), None)
    return jax.shard_map(body, mesh=mesh, in_specs=in_specs, out_specs=out_specs, check_vma=False)
```

```python
import functools

import jax
import jax.numpy as jnp
from jax import lax
from jax.experimental import pallas as pl
from jax.experimental.pallas import tpu as pltpu
from jax.sharding import PartitionSpec as P


HEAD_SIZE = 128

epsilon = 1e-05
rope_base = 500000.0
masked = -1e30
initial_peak = -1e29
ROWS = 256
SLOTS = 4
PIECE_SPACE = pltpu.HBM
exp2_scale = 1.4426950408889634 * HEAD_SIZE ** (-0.5)

RING = 4
RELATIVE = (0, 3, 1, 2)


def ring_shift(step):
    return [(i, (i + step) % RING) for i in range(RING)]


def plane_shift(step, first_axis):
    pairs = []
    for d in range(32):
        x, z, core = d // 8, d // 2 % 4, d % 2
        if (core == 0) == first_axis:
            z = (z + step) % 4
        else:
            x = (x + step) % 4
        pairs.append((d, x * 8 + z * 2 + core))
    return pairs


CORE_SWAP = [(d, d ^ 1) for d in range(32)]


def ring_gather(piece, axis, shift):
    half = piece.shape[0] // 2
    behind = lax.ppermute(piece, axis, shift(1))
    ahead = lax.ppermute(piece, axis, shift(-1))
    upper = lax.ppermute(behind[:half], axis, shift(1))
    lower = lax.ppermute(ahead[half:], axis, shift(-1))
    return [piece, behind, ahead, upper, lower]


def gather_plane(keys, values):
    core = lax.axis_index("dp") & 1
    other = lax.ppermute(jnp.where(core == 0, values, keys), "dp", CORE_SWAP)
    mine = jnp.where(
        core == 0,
        jnp.concatenate([keys, other], axis=0),
        jnp.concatenate([other, values], axis=0),
    )
    line = [mine] + [lax.ppermute(mine, "dp", plane_shift(n, True)) for n in (1, -1, 2)]
    shift = functools.partial(plane_shift, first_axis=False)
    plane = ring_gather(jnp.concatenate(line, axis=0), "dp", shift)
    traded = [lax.ppermute(piece, "dp", CORE_SWAP) for piece in plane[:3]]
    traded += [lax.ppermute(piece, "dp", CORE_SWAP) for piece in plane[3:]]
    return plane + traded


def doc_starts(lengths, positions):
    order = jnp.arange(lengths.shape[0], dtype=jnp.int32)
    doc_ends = jnp.sum(jnp.where(order[:, None] <= order[None, :], lengths[:, None], 0), axis=0)
    closed = (doc_ends[None, :] <= positions[:, None]).astype(jnp.int32)
    return jnp.sum(closed * lengths[None, :], axis=1)


def angles_of(offsets):
    lane = jnp.arange(HEAD_SIZE, dtype=jnp.int32)
    half_width = HEAD_SIZE // 2
    exponent = (lane & (half_width - 1)).astype(jnp.float32) * (-2.0 / HEAD_SIZE)
    frequency = rope_base**exponent
    angles = offsets.astype(jnp.float32)[:, None] * frequency[None, :]
    sign = jnp.where(lane < half_width, -1.0, 1.0).astype(jnp.float32)
    return jnp.cos(angles), jnp.sin(angles) * sign[None, :]


def norm(tokens, norm_gain):
    wide = tokens.astype(jnp.float32)
    inverse = lax.rsqrt(jnp.mean(wide * wide, axis=1, keepdims=True) + epsilon)
    return (wide * inverse * norm_gain[None, :]).astype(jnp.bfloat16)


def wide_dot(a, b):
    return jnp.dot(a, b, preferred_element_type=jnp.float32)


def attend_kernel(ids, lengths, query, cos_part, sin_part, *refs, quarters):
    pieces, refs = refs[:10], refs[10:]
    out, rows, scores, peak, summed, starts, query_at, key_at, block, sems = refs
    count = query.shape[0]
    heads = query.shape[1] // HEAD_SIZE
    size = block.shape[2]
    span = count // len(quarters)
    docs = lengths.shape[0]
    dp, mine = ids[0], ids[1]
    own_x, own_z, core = dp >> 3, (dp >> 1) & 3, dp & 1

    def quarter_base(quarter):
        return ((mine + RELATIVE[quarter]) & 3) * span

    bases = [dp * (RING * span) + quarter_base(q) for q in quarters]
    first = functools.reduce(jnp.minimum, bases)
    last = functools.reduce(jnp.maximum, bases) + (span - 1)
    ends, end = [], jnp.int32(0)
    for d in range(docs):
        end = end + lengths[d]
        ends.append(end)

    def start_of(at):
        start = jnp.zeros_like(at)
        for end in ends:
            start = jnp.where(at >= end, end, start)
        return start

    first_start, last_start = start_of(first), start_of(last)
    low, high = first_start // size, last // size + 1
    full_low, full_high = (last_start + size - 1) // size, (first + 1) // size

    def place(step):
        return jnp.where(step == 0, 0, jnp.where(step == 1, 2, jnp.where(step == 2, 3, 1)))

    def start_copies(chip):
        slot = chip & (SLOTS - 1)
        at_x, at_z = place(((chip >> 2) - own_x) & 3), place(((chip & 3) - own_z) & 3)
        outer = jnp.where(core == 0, at_x, at_z)
        inner = jnp.where(core == 0, at_z, at_x)
        for side, kind, major, minor in ((0, core, outer, inner), (5, 1 - core, inner, outer)):
            index = jnp.where((major == 3) & (minor >= 2), 4, major)
            line = jnp.where(major == 3, minor & 1, minor)
            for n in range(5):

                @pl.when(index == n)
                def _():
                    pltpu.make_async_copy(
                        pieces[side + n].at[pl.ds(pl.multiple_of(line * size, size), size)],
                        block.at[slot, kind],
                        sems.at[slot, kind],
                    ).start()

    def wait_copies(chip):
        slot = chip & (SLOTS - 1)
        for kind in range(2):
            pltpu.make_async_copy(
                pieces[0].at[pl.ds(0, size)], block.at[slot, kind], sems.at[slot, kind]
            ).wait()

    def begin(chip, carry):
        start_copies(chip)
        return carry

    lax.fori_loop(low, jnp.minimum(low + (SLOTS - 1), high), begin, 0)
    here = slice(quarters[0] * span, quarters[0] * span + count)
    for h in range(heads):
        at = slice(h * HEAD_SIZE, (h + 1) * HEAD_SIZE)
        head = query[:, at]
        turned = head * cos_part[here, :] + pltpu.roll(head, HEAD_SIZE // 2, 1) * sin_part[here, :]
        rows[h * count : (h + 1) * count, :] = turned.astype(jnp.bfloat16)
    for i, base in enumerate(bases):
        at = base + lax.broadcasted_iota(jnp.int32, (span, 1), 0)
        query_at[i * span : (i + 1) * span, :] = at
        starts[i * span : (i + 1) * span, :] = start_of(at)
    for i in range(size // span):
        base = (i // RING) * (RING * span) + quarter_base(i % RING)
        lane = lax.broadcasted_iota(jnp.int32, (1, span), 1)
        key_at[:, i * span : (i + 1) * span] = base + lane
    peak[...] = jnp.full(peak.shape, initial_peak, jnp.float32)
    summed[...] = jnp.zeros(summed.shape, jnp.float32)

    def score(chip, at):
        scores[at, :] = lax.dot_general(
            rows[at, :],
            block[chip & (SLOTS - 1), 0],
            (((1,), (1,)), ((), ())),
            preferred_element_type=jnp.float32,
        )

    def step(chip, cut):
        slot = chip & (SLOTS - 1)
        block_values = jnp.concatenate(
            [block[slot, 1], jnp.ones((size, HEAD_SIZE), jnp.bfloat16)], axis=1
        )
        if cut:
            where = chip * size + key_at[...]
            scores_seen = (where >= starts[...]) & (where <= query_at[...])
            if count < ROWS:
                scores_seen = jnp.concatenate([scores_seen] * (ROWS // count), axis=0)
        for r in range(heads * count // ROWS):
            at = slice(r * ROWS, (r + 1) * ROWS)
            local = (r * ROWS) % max(count, ROWS)

            def part(c):
                here = scores[at, c : c + HEAD_SIZE]
                if cut:
                    here = jnp.where(
                        scores_seen[local : local + ROWS, c : c + HEAD_SIZE], here, masked
                    )
                return here

            old = peak[at, :]
            columns = range(0, size, HEAD_SIZE)
            best = functools.reduce(jnp.maximum, [part(c) for c in columns])
            fresh = jnp.maximum(old, jnp.max(best, axis=1, keepdims=True))
            peak[at, :] = fresh
            shrink = jnp.exp2((old - fresh) * exp2_scale)
            probs = [jnp.exp2((part(c) - fresh) * exp2_scale).astype(jnp.bfloat16) for c in columns]
            update = wide_dot(jnp.concatenate(probs, axis=1), block_values)
            summed[at, :HEAD_SIZE] = summed[at, :HEAD_SIZE] * shrink + update[:, :HEAD_SIZE]
            summed[at, HEAD_SIZE:] = summed[at, HEAD_SIZE:] * shrink + update[:, HEAD_SIZE:]
            score(chip + 1, at)

    def one_block(chip, carry):
        @pl.when(chip + 1 < high)
        def _():
            wait_copies(chip + 1)

        @pl.when(chip + (SLOTS - 1) < high)
        def _():
            start_copies(chip + (SLOTS - 1))

        whole = (chip >= full_low) & (chip < full_high)

        @pl.when(whole)
        def _():
            step(chip, False)

        @pl.when(jnp.logical_not(whole))
        def _():
            step(chip, True)

        return carry

    wait_copies(low)
    for r in range(heads * count // ROWS):
        score(low, slice(r * ROWS, (r + 1) * ROWS))
    lax.fori_loop(low, high, one_block, 0)
    for h in range(heads):
        at = slice(h * count, (h + 1) * count)
        attended = summed[at, :HEAD_SIZE] / summed[at, HEAD_SIZE:]
        out[:, h * HEAD_SIZE : (h + 1) * HEAD_SIZE] = attended.astype(jnp.bfloat16)


def attend(ids, lengths, query, cos_part, sin_part, pieces, quarters):
    count, width = query.shape
    rows = count * width // HEAD_SIZE
    size = 2 * RING * count // len(quarters)
    vmem = pl.BlockSpec(memory_space=pltpu.VMEM)
    smem = pl.BlockSpec(memory_space=pltpu.SMEM)
    hbm = pl.BlockSpec(memory_space=PIECE_SPACE)
    return pl.pallas_call(
        functools.partial(attend_kernel, quarters=quarters),
        out_shape=jax.ShapeDtypeStruct((count, width), jnp.bfloat16),
        in_specs=[smem, smem, vmem, vmem, vmem] + [hbm] * 10,
        out_specs=vmem,
        scratch_shapes=[
            pltpu.VMEM((rows, HEAD_SIZE), jnp.bfloat16),
            pltpu.VMEM((rows, size), jnp.float32),
            pltpu.VMEM((rows, HEAD_SIZE), jnp.float32),
            pltpu.VMEM((rows, 2 * HEAD_SIZE), jnp.float32),
            pltpu.VMEM((count, 1), jnp.int32),
            pltpu.VMEM((count, 1), jnp.int32),
            pltpu.VMEM((1, size), jnp.int32),
            pltpu.VMEM((SLOTS, 2, size, HEAD_SIZE), jnp.bfloat16),
            pltpu.SemaphoreType.DMA((SLOTS, 2)),
        ],
        compiler_params=pltpu.CompilerParams(vmem_limit_bytes=32 * 2**20),
        cost_estimate=pl.CostEstimate(
            flops=rows * 4096 * 512, transcendentals=rows * 4096, bytes_accessed=4 << 20
        ),
        name="attend",
    )(ids, lengths, query, cos_part, sin_part, *pieces)


def body(tokens, norm_gain, w_query, key_weight, value_weight, w_out, lengths):
    count = tokens.shape[0]
    dp, mine = lax.axis_index("dp"), lax.axis_index("tensor")
    normed = norm(tokens, norm_gain)
    quarter = (mine + jnp.array(RELATIVE, jnp.int32)) & 3
    local = (quarter[:, None] * count + jnp.arange(count, dtype=jnp.int32)[None, :]).reshape(-1)
    positions = dp * (RING * count) + local
    cos_part, sin_part = angles_of(positions - doc_starts(lengths, positions))
    ids = jnp.stack([dp, mine]).astype(jnp.int32)

    def project(piece, first):
        at = slice(first, first + piece.shape[0])
        key = wide_dot(piece, key_weight)
        key = key * cos_part[at] + jnp.roll(key, HEAD_SIZE // 2, axis=1) * sin_part[at]
        value = wide_dot(piece, value_weight)
        return key.astype(jnp.bfloat16), value.astype(jnp.bfloat16)

    half = count // 2
    query = [None] * RING
    kv_own = project(normed, 0)
    query[0] = wide_dot(normed, w_query)
    behind_top = lax.ppermute(normed[:half], "tensor", ring_shift(1))
    ahead_low = lax.ppermute(normed[half:], "tensor", ring_shift(-1))
    behind_low = lax.ppermute(normed[half:], "tensor", ring_shift(1))
    ahead_top = lax.ppermute(normed[:half], "tensor", ring_shift(-1))
    far_top = lax.ppermute(behind_top, "tensor", ring_shift(1))
    far_low = lax.ppermute(ahead_low, "tensor", ring_shift(-1))
    behind_low, ahead_top, query[0], kv_own, ids = lax.optimization_barrier(
        (behind_low, ahead_top, query[0], kv_own, ids)
    )
    behind = jnp.concatenate([behind_top, behind_low], axis=0)
    ahead = jnp.concatenate([ahead_top, ahead_low], axis=0)
    kv_behind, kv_ahead = project(behind, count), project(ahead, 2 * count)
    near = [wide_dot(behind, w_query), wide_dot(ahead, w_query)]
    far_top, far_low, kv_behind, kv_ahead, near = lax.optimization_barrier(
        (far_top, far_low, kv_behind, kv_ahead, near)
    )
    far = jnp.concatenate([far_top, far_low], axis=0)
    kv = (kv_own, kv_behind, kv_ahead, project(far, 3 * count))
    pieces = gather_plane(*[jnp.concatenate(a, axis=0) for a in zip(*kv)])
    query[3] = wide_dot(far, w_query)
    near_rows = jnp.concatenate(near, axis=0)

    def branch(quarters, after=None):
        rows = near_rows if len(quarters) == 2 else query[quarters[0]]
        if after is not None:
            rows, after = lax.optimization_barrier((rows, after))
        attended = attend(ids, lengths, rows, cos_part, sin_part, pieces, quarters)
        return wide_dot(attended, w_out), after

    half = w_out.shape[1] // 2
    far, _ = branch((3,))
    far = far.astype(jnp.bfloat16)
    near, far = branch((1, 2), far)
    from_behind = lax.ppermute(far[:, :half], "tensor", ring_shift(1))
    from_ahead = lax.ppermute(far[:, half:], "tensor", ring_shift(-1))
    to_behind, to_ahead = near[:count], near[count:]
    plain_up = to_ahead[:, half:].astype(jnp.bfloat16)
    plain_up = lax.ppermute(plain_up, "tensor", ring_shift(1))
    plain_down = to_behind[:, :half].astype(jnp.bfloat16)
    plain_down = lax.ppermute(plain_down, "tensor", ring_shift(-1))
    sum_up = (to_ahead[:, :half] + from_behind.astype(jnp.float32)).astype(jnp.bfloat16)
    sum_down = (to_behind[:, half:] + from_ahead.astype(jnp.float32)).astype(jnp.bfloat16)
    here, (sum_up, sum_down) = branch((0,), (sum_up, sum_down))
    sum_up = lax.ppermute(sum_up, "tensor", ring_shift(1))
    sum_down = lax.ppermute(sum_down, "tensor", ring_shift(-1))
    wide = [a.astype(jnp.float32) for a in (sum_up, plain_down, plain_up, sum_down)]
    total = here + jnp.concatenate([wide[0] + wide[1], wide[2] + wide[3]], axis=1)
    return (tokens.astype(jnp.float32) + total).astype(jnp.bfloat16)


def solution(mesh):
    in_specs = (
        P(("dp", "tensor"), None),
        P(),
        P(None, "tensor"),
        P(None, "tensor"),
        P(None, "tensor"),
        P("tensor", None),
        P(),
    )
    out_specs = P(("dp", "tensor"), None)
    return jax.shard_map(body, mesh=mesh, in_specs=in_specs, out_specs=out_specs, check_vma=False)
```

```python
import functools

import jax
import jax.numpy as jnp
from jax import lax
from jax.experimental import pallas as pl
from jax.experimental.pallas import tpu as pltpu
from jax.sharding import PartitionSpec as P


HEAD_SIZE = 128

epsilon = 1e-05
rope_base = 500000.0
masked = -1e30
initial_peak = -1e29
ROWS = 256
SLOTS = 4
PIECE_SPACE = pltpu.HBM
exp2_scale = 1.4426950408889634 * HEAD_SIZE ** (-0.5)

RING = 4
RELATIVE = (0, 3, 1, 2)


def ring_shift(step):
    return [(i, (i + step) % RING) for i in range(RING)]


def plane_shift(step, first_axis):
    pairs = []
    for d in range(32):
        x, z, core = d // 8, d // 2 % 4, d % 2
        if (core == 0) == first_axis:
            z = (z + step) % 4
        else:
            x = (x + step) % 4
        pairs.append((d, x * 8 + z * 2 + core))
    return pairs


CORE_SWAP = [(d, d ^ 1) for d in range(32)]


def ring_gather(piece, axis, shift):
    half = piece.shape[0] // 2
    behind = lax.ppermute(piece, axis, shift(1))
    ahead = lax.ppermute(piece, axis, shift(-1))
    upper = lax.ppermute(behind[:half], axis, shift(1))
    lower = lax.ppermute(ahead[half:], axis, shift(-1))
    return [piece, behind, ahead, upper, lower]


def gather_plane(keys, values):
    core = lax.axis_index("dp") & 1
    other = lax.ppermute(jnp.where(core == 0, values, keys), "dp", CORE_SWAP)
    mine = jnp.where(
        core == 0,
        jnp.concatenate([keys, other], axis=0),
        jnp.concatenate([other, values], axis=0),
    )
    line = [mine] + [lax.ppermute(mine, "dp", plane_shift(n, True)) for n in (1, -1, 2)]
    shift = functools.partial(plane_shift, first_axis=False)
    plane = ring_gather(jnp.concatenate(line, axis=0), "dp", shift)
    traded = [lax.ppermute(piece, "dp", CORE_SWAP) for piece in plane[:3]]
    traded += [lax.ppermute(piece, "dp", CORE_SWAP) for piece in plane[3:]]
    return plane + traded


def doc_starts(lengths, positions):
    order = jnp.arange(lengths.shape[0], dtype=jnp.int32)
    doc_ends = jnp.sum(jnp.where(order[:, None] <= order[None, :], lengths[:, None], 0), axis=0)
    closed = (doc_ends[None, :] <= positions[:, None]).astype(jnp.int32)
    return jnp.sum(closed * lengths[None, :], axis=1)


def angles_of(offsets):
    lane = jnp.arange(HEAD_SIZE, dtype=jnp.int32)
    half_width = HEAD_SIZE // 2
    exponent = (lane & (half_width - 1)).astype(jnp.float32) * (-2.0 / HEAD_SIZE)
    frequency = rope_base**exponent
    angles = offsets.astype(jnp.float32)[:, None] * frequency[None, :]
    sign = jnp.where(lane < half_width, -1.0, 1.0).astype(jnp.float32)
    return jnp.cos(angles), jnp.sin(angles) * sign[None, :]


def norm_kernel(tokens, gain, normed, top, low):
    count = tokens.shape[0]
    half = count // 2
    for at in range(0, count, 16):
        wide = tokens[at : at + 16, :].astype(jnp.float32)
        inverse = lax.rsqrt(jnp.mean(wide * wide, axis=1, keepdims=True) + epsilon)
        rows = (wide * inverse * gain[...]).astype(jnp.bfloat16)
        normed[at : at + 16, :] = rows
        if at < half:
            top[at : at + 16, :] = rows
        else:
            low[at - half : at - half + 16, :] = rows


def norm(tokens, norm_gain):
    count, width = tokens.shape
    vmem = pl.BlockSpec(memory_space=pltpu.VMEM)
    shapes = [(count, width), (count // 2, width), (count // 2, width)]
    return pl.pallas_call(
        norm_kernel,
        out_shape=[jax.ShapeDtypeStruct(shape, jnp.bfloat16) for shape in shapes],
        in_specs=[vmem, vmem],
        out_specs=[vmem] * 3,
        compiler_params=pltpu.CompilerParams(vmem_limit_bytes=16 * 2**20),
        name="norm",
    )(tokens, norm_gain[None, :])


def wide_dot(a, b):
    return jnp.dot(a, b, preferred_element_type=jnp.float32)


def attend_kernel(ids, lengths, query, cos_part, sin_part, *refs, quarters):
    pieces, refs = refs[:10], refs[10:]
    out, rows, scores, peak, summed, starts, query_at, key_at, block, sems = refs
    count = query.shape[0]
    heads = query.shape[1] // HEAD_SIZE
    size = block.shape[2]
    span = count // len(quarters)
    docs = lengths.shape[0]
    dp, mine = ids[0], ids[1]
    own_x, own_z, core = dp >> 3, (dp >> 1) & 3, dp & 1

    def quarter_base(quarter):
        return ((mine + RELATIVE[quarter]) & 3) * span

    bases = [dp * (RING * span) + quarter_base(q) for q in quarters]
    first = functools.reduce(jnp.minimum, bases)
    last = functools.reduce(jnp.maximum, bases) + (span - 1)
    ends, end = [], jnp.int32(0)
    for d in range(docs):
        end = end + lengths[d]
        ends.append(end)

    def start_of(at):
        start = jnp.zeros_like(at)
        for end in ends:
            start = jnp.where(at >= end, end, start)
        return start

    first_start, last_start = start_of(first), start_of(last)
    low, high = first_start // size, last // size + 1
    full_low, full_high = (last_start + size - 1) // size, (first + 1) // size

    def place(step):
        return jnp.where(step == 0, 0, jnp.where(step == 1, 2, jnp.where(step == 2, 3, 1)))

    def start_copies(chip):
        slot = chip & (SLOTS - 1)
        at_x, at_z = place(((chip >> 2) - own_x) & 3), place(((chip & 3) - own_z) & 3)
        outer = jnp.where(core == 0, at_x, at_z)
        inner = jnp.where(core == 0, at_z, at_x)
        for side, kind, major, minor in ((0, core, outer, inner), (5, 1 - core, inner, outer)):
            index = jnp.where((major == 3) & (minor >= 2), 4, major)
            line = jnp.where(major == 3, minor & 1, minor)
            for n in range(5):

                @pl.when(index == n)
                def _():
                    pltpu.make_async_copy(
                        pieces[side + n].at[pl.ds(pl.multiple_of(line * size, size), size)],
                        block.at[slot, kind],
                        sems.at[slot, kind],
                    ).start()

    def wait_copies(chip):
        slot = chip & (SLOTS - 1)
        for kind in range(2):
            pltpu.make_async_copy(
                pieces[0].at[pl.ds(0, size)], block.at[slot, kind], sems.at[slot, kind]
            ).wait()

    def begin(chip, carry):
        start_copies(chip)
        return carry

    lax.fori_loop(low, jnp.minimum(low + (SLOTS - 1), high), begin, 0)
    here = slice(quarters[0] * span, quarters[0] * span + count)
    for h in range(heads):
        at = slice(h * HEAD_SIZE, (h + 1) * HEAD_SIZE)
        head = query[:, at]
        turned = head * cos_part[here, :] + pltpu.roll(head, HEAD_SIZE // 2, 1) * sin_part[here, :]
        rows[h * count : (h + 1) * count, :] = turned.astype(jnp.bfloat16)
    for i, base in enumerate(bases):
        at = base + lax.broadcasted_iota(jnp.int32, (span, 1), 0)
        query_at[i * span : (i + 1) * span, :] = at
        starts[i * span : (i + 1) * span, :] = start_of(at)
    for i in range(size // span):
        base = (i // RING) * (RING * span) + quarter_base(i % RING)
        lane = lax.broadcasted_iota(jnp.int32, (1, span), 1)
        key_at[:, i * span : (i + 1) * span] = base + lane
    peak[...] = jnp.full(peak.shape, initial_peak, jnp.float32)
    summed[...] = jnp.zeros(summed.shape, jnp.float32)

    def score(chip, at):
        scores[at, :] = lax.dot_general(
            rows[at, :],
            block[chip & (SLOTS - 1), 0],
            (((1,), (1,)), ((), ())),
            preferred_element_type=jnp.float32,
        )

    def step(chip, cut):
        slot = chip & (SLOTS - 1)
        block_values = jnp.concatenate(
            [block[slot, 1], jnp.ones((size, HEAD_SIZE), jnp.bfloat16)], axis=1
        )
        if cut:
            where = chip * size + key_at[...]
            scores_seen = (where >= starts[...]) & (where <= query_at[...])
            if count < ROWS:
                scores_seen = jnp.concatenate([scores_seen] * (ROWS // count), axis=0)
        for r in range(heads * count // ROWS):
            at = slice(r * ROWS, (r + 1) * ROWS)
            local = (r * ROWS) % max(count, ROWS)

            columns = range(0, size, HEAD_SIZE)
            old, best = peak[at, :], None
            for c in columns:
                part = scores[at, c : c + HEAD_SIZE]
                if cut:
                    seen = scores_seen[local : local + ROWS, c : c + HEAD_SIZE]
                    part = jnp.where(seen, part, masked)
                    scores[at, c : c + HEAD_SIZE] = part
                best = part if best is None else jnp.maximum(best, part)
            fresh = jnp.maximum(old, jnp.max(best, axis=1, keepdims=True))
            peak[at, :] = fresh
            shrink = jnp.exp2((old - fresh) * exp2_scale)
            probs = [
                jnp.exp2((scores[at, c : c + HEAD_SIZE] - fresh) * exp2_scale).astype(jnp.bfloat16)
                for c in columns
            ]
            update = wide_dot(jnp.concatenate(probs, axis=1), block_values)
            summed[at, :HEAD_SIZE] = summed[at, :HEAD_SIZE] * shrink + update[:, :HEAD_SIZE]
            summed[at, HEAD_SIZE:] = summed[at, HEAD_SIZE:] * shrink + update[:, HEAD_SIZE:]
            score(chip + 1, at)

    def one_block(chip, carry):
        @pl.when(chip + 1 < high)
        def _():
            wait_copies(chip + 1)

        @pl.when(chip + (SLOTS - 1) < high)
        def _():
            start_copies(chip + (SLOTS - 1))

        whole = (chip >= full_low) & (chip < full_high)

        @pl.when(whole)
        def _():
            step(chip, False)

        @pl.when(jnp.logical_not(whole))
        def _():
            step(chip, True)

        return carry

    wait_copies(low)
    for r in range(heads * count // ROWS):
        score(low, slice(r * ROWS, (r + 1) * ROWS))
    lax.fori_loop(low, high, one_block, 0)
    for h in range(heads):
        at = slice(h * count, (h + 1) * count)
        attended = summed[at, :HEAD_SIZE] / summed[at, HEAD_SIZE:]
        out[:, h * HEAD_SIZE : (h + 1) * HEAD_SIZE] = attended.astype(jnp.bfloat16)


def attend(ids, lengths, query, cos_part, sin_part, pieces, quarters):
    count, width = query.shape
    rows = count * width // HEAD_SIZE
    size = 2 * RING * count // len(quarters)
    vmem = pl.BlockSpec(memory_space=pltpu.VMEM)
    smem = pl.BlockSpec(memory_space=pltpu.SMEM)
    hbm = pl.BlockSpec(memory_space=PIECE_SPACE)
    return pl.pallas_call(
        functools.partial(attend_kernel, quarters=quarters),
        out_shape=jax.ShapeDtypeStruct((count, width), jnp.bfloat16),
        in_specs=[smem, smem, vmem, vmem, vmem] + [hbm] * 10,
        out_specs=vmem,
        scratch_shapes=[
            pltpu.VMEM((rows, HEAD_SIZE), jnp.bfloat16),
            pltpu.VMEM((rows, size), jnp.float32),
            pltpu.VMEM((rows, HEAD_SIZE), jnp.float32),
            pltpu.VMEM((rows, 2 * HEAD_SIZE), jnp.float32),
            pltpu.VMEM((count, 1), jnp.int32),
            pltpu.VMEM((count, 1), jnp.int32),
            pltpu.VMEM((1, size), jnp.int32),
            pltpu.VMEM((SLOTS, 2, size, HEAD_SIZE), jnp.bfloat16),
            pltpu.SemaphoreType.DMA((SLOTS, 2)),
        ],
        compiler_params=pltpu.CompilerParams(vmem_limit_bytes=32 * 2**20),
        cost_estimate=pl.CostEstimate(
            flops=rows * 4096 * 512, transcendentals=rows * 4096, bytes_accessed=4 << 20
        ),
        name="attend",
    )(ids, lengths, query, cos_part, sin_part, *pieces)


def body(tokens, norm_gain, w_query, key_weight, value_weight, w_out, lengths):
    count = tokens.shape[0]
    dp, mine = lax.axis_index("dp"), lax.axis_index("tensor")
    normed, normed_top, normed_low = norm(tokens, norm_gain)
    quarter = (mine + jnp.array(RELATIVE, jnp.int32)) & 3
    local = (quarter[:, None] * count + jnp.arange(count, dtype=jnp.int32)[None, :]).reshape(-1)
    positions = dp * (RING * count) + local
    cos_part, sin_part = angles_of(positions - doc_starts(lengths, positions))
    ids = jnp.stack([dp, mine]).astype(jnp.int32)

    def project(piece, first):
        at = slice(first, first + piece.shape[0])
        key = wide_dot(piece, key_weight)
        key = key * cos_part[at] + jnp.roll(key, HEAD_SIZE // 2, axis=1) * sin_part[at]
        value = wide_dot(piece, value_weight)
        return key.astype(jnp.bfloat16), value.astype(jnp.bfloat16)

    half = count // 2
    query = [None] * RING
    kv_own = project(normed, 0)
    query[0] = wide_dot(normed, w_query)
    behind_top = lax.ppermute(normed_top, "tensor", ring_shift(1))
    ahead_low = lax.ppermute(normed_low, "tensor", ring_shift(-1))
    behind_low = lax.ppermute(normed_low, "tensor", ring_shift(1))
    ahead_top = lax.ppermute(normed_top, "tensor", ring_shift(-1))
    far_top = lax.ppermute(behind_top, "tensor", ring_shift(1))
    far_low = lax.ppermute(ahead_low, "tensor", ring_shift(-1))
    behind_low, ahead_top, query[0], kv_own, ids = lax.optimization_barrier(
        (behind_low, ahead_top, query[0], kv_own, ids)
    )
    behind = jnp.concatenate([behind_top, behind_low], axis=0)
    ahead = jnp.concatenate([ahead_top, ahead_low], axis=0)
    kv_behind, kv_ahead = project(behind, count), project(ahead, 2 * count)
    near = [wide_dot(behind, w_query), wide_dot(ahead, w_query)]
    far_top, far_low, kv_behind, kv_ahead, near = lax.optimization_barrier(
        (far_top, far_low, kv_behind, kv_ahead, near)
    )
    far = jnp.concatenate([far_top, far_low], axis=0)
    kv = (kv_own, kv_behind, kv_ahead, project(far, 3 * count))
    pieces = gather_plane(*[jnp.concatenate(a, axis=0) for a in zip(*kv)])
    query[3] = wide_dot(far, w_query)
    near_rows = jnp.concatenate(near, axis=0)

    def branch(quarters, after=None):
        rows = near_rows if len(quarters) == 2 else query[quarters[0]]
        if after is not None:
            rows, after = lax.optimization_barrier((rows, after))
        attended = attend(ids, lengths, rows, cos_part, sin_part, pieces, quarters)
        return wide_dot(attended, w_out), after

    half = w_out.shape[1] // 2
    far, _ = branch((3,))
    far = far.astype(jnp.bfloat16)
    near, far = branch((1, 2), far)
    from_behind = lax.ppermute(far[:, :half], "tensor", ring_shift(1))
    from_ahead = lax.ppermute(far[:, half:], "tensor", ring_shift(-1))
    to_behind, to_ahead = near[:count], near[count:]
    plain_up = to_ahead[:, half:].astype(jnp.bfloat16)
    plain_up = lax.ppermute(plain_up, "tensor", ring_shift(1))
    plain_down = to_behind[:, :half].astype(jnp.bfloat16)
    plain_down = lax.ppermute(plain_down, "tensor", ring_shift(-1))
    sum_up = (to_ahead[:, :half] + from_behind.astype(jnp.float32)).astype(jnp.bfloat16)
    sum_down = (to_behind[:, half:] + from_ahead.astype(jnp.float32)).astype(jnp.bfloat16)
    here, (sum_up, sum_down) = branch((0,), (sum_up, sum_down))
    sum_up = lax.ppermute(sum_up, "tensor", ring_shift(1))
    sum_down = lax.ppermute(sum_down, "tensor", ring_shift(-1))
    wide = [a.astype(jnp.float32) for a in (sum_up, plain_down, plain_up, sum_down)]
    total = here + jnp.concatenate([wide[0] + wide[1], wide[2] + wide[3]], axis=1)
    return (tokens.astype(jnp.float32) + total).astype(jnp.bfloat16)


def solution(mesh):
    in_specs = (
        P(("dp", "tensor"), None),
        P(),
        P(None, "tensor"),
        P(None, "tensor"),
        P(None, "tensor"),
        P("tensor", None),
        P(),
    )
    out_specs = P(("dp", "tensor"), None)
    return jax.shard_map(body, mesh=mesh, in_specs=in_specs, out_specs=out_specs, check_vma=False)
```
